32 devices in a mesh: ga: 2 (over y), gx: 4 (over z), gy: 2 (over x), col: 2 (over core).
Axes of the slice: x: 2, y: 2, z: 4, core: 2. Of those that a mesh axis runs over, the one named last changes fastest.
Arguments:
- pair_rep: bfloat16 [2, 160, 160, 128], P('ga', 'gx', 'gy'), parts along dimension 0, may hold values from -6 to 6
- pair_mask: int32 [2, 160, 160], P('ga', 'gx', 'gy'), parts along dimension 0, may hold values 0 or 1
- amax_history: float32 [2, 128], P(None, 'col'), may hold values from 0.3 to 3
- in_gain: float32 [128], replicated, may hold values from 0.5 to 1.5
- in_bias: float32 [128], replicated, may hold values from -3 to 3
- proj_weight: bfloat16 [128, 4, 128], P(None, None, 'col'), may hold values from -0.5 to 0.5
- gate_weight: bfloat16 [128, 128], P(None, 'col'), may hold values from -0.5 to 0.5
- out_gain: float32 [128], replicated, may hold values from 0.5 to 1.5
- out_bias: float32 [128], replicated, may hold values from -3 to 3
- out_weight: bfloat16 [128, 128], P(None, 'col'), may hold values from -0.5 to 0.5
Outputs:
- update: bfloat16 [2, 160, 160, 128], P('ga', 'gx', 'gy', 'col'), parts along dimension 0
- new_amax: float32 [4, 128], P('ga', 'col'), parts along dimension 0
The draws below stay inside these ranges and needn't reach their ends.
There are 2 independent parts, one for each index of `ga`. The reference program is written for one: setup_inputs(seed, part) draws one part's arguments, and reference() takes and returns one part's arrays. A program takes and returns all parts, laid end to end along the dimension named above; an argument that names none is the same for every part. Nothing has to cross between parts.
All inputs are finite; a program needn't handle non-finite values. No bound on the sum of `pair_mask` on one device may be relied on, other than what follows from the above.
Results may differ from the reference program's by a relative error of at most 0.0065.
Values may be sent and summed in bfloat16 or wider, within the bound.
A program may use at most 128 MiB of HBM per device.

```python
import math
import jax
import jax.numpy as jnp
from jax import lax

C = 128
CROPS = 1
N = 160


def place_ends(result, stream_key, low, top_value):
    longest = result.shape.index(max(result.shape))
    spots = []
    for shift in (0, 1):
        where = [jax.random.randint(jax.random.fold_in(stream_key, axis), (), 0, length) for axis, length in enumerate(result.shape)]
        where[longest] = (where[longest] + shift) % result.shape[longest]
        spots.append(tuple(where))
    return result.at[spots[0]].set(low).at[spots[1]].set(top_value)


def levels(key, shape, cuts, low, largest):
    level, own = 1.0, jax.random.fold_in(key, 6)
    for axis_at, blocks in cuts:
        heights = jnp.exp(jax.random.uniform(jax.random.fold_in(own, axis_at), (blocks,), jnp.float32, low / len(cuts), largest / len(cuts)))
        level = level * jnp.repeat(heights, shape[axis_at] // blocks).reshape([-1 if axis == axis_at else 1 for axis in range(len(shape))])
    return level


def scatter_about(own_key, extent, scale, reach, pieces=(), held_as=jnp.bfloat16):
    result = scale * jax.random.normal(own_key, extent, jnp.float32)
    if pieces:
        result = result * levels(own_key, extent, pieces, -0.22, 0.18)
    return jnp.clip(result, -reach, reach).astype(held_as)


def setup_inputs(seed: int = 0, part: int = 0) -> dict:
    seeds = jax.random.split(jax.random.key(seed), 11)
    part_keys = jax.random.split(jax.random.fold_in(seeds[10], part), 11)
    pair_rep = scatter_about(part_keys[0], (CROPS, N, N, C), 1.0, 6.0, ((1, 4), (2, 2)))
    pair_mask = place_ends((jax.random.randint(part_keys[1], (CROPS, N, N), 0, 10) < 9).astype(jnp.int32), jax.random.fold_in(part_keys[1], 1), 0, 1)
    amax_history = jnp.clip(jnp.exp(math.log(3.0) - 2.3025851 * jax.random.uniform(seeds[2], (2, C), jnp.float32) ** levels(seeds[2], (2, C), ((1, 2),), -0.2, 0.2)), 0.3, 3.0)
    in_gain = jnp.clip(1.0 + 0.1 * jax.random.normal(seeds[3], (C,), jnp.float32), 0.5, 1.5)
    in_bias = scatter_about(seeds[4], (C,), 0.5, 3.0, (), jnp.float32)
    proj_weight = scatter_about(seeds[5], (C, 4, C), C ** -0.5, 0.5, ((2, 2),))
    gate_weight = scatter_about(seeds[6], (C, C), C ** -0.5, 0.5, ((1, 2),))
    out_gain = jnp.clip(1.0 + 0.1 * jax.random.normal(seeds[7], (C,), jnp.float32), 0.5, 1.5)
    out_bias = scatter_about(seeds[8], (C,), 0.5, 3.0, (), jnp.float32)
    out_weight = scatter_about(seeds[9], (C, C), C ** -0.5, 0.5, ((1, 2),))
    return {"pair_rep": pair_rep, "pair_mask": pair_mask, "amax_history": amax_history, "in_gain": in_gain, "in_bias": in_bias, "proj_weight": proj_weight, "gate_weight": gate_weight, "out_gain": out_gain, "out_bias": out_bias, "out_weight": out_weight}


epsilon = 1e-05
format_limit = 448.0

def layer_norm(values, gain, bias):
    average = lax.optimization_barrier(jnp.mean(values, axis=-1, keepdims=True))
    spread = lax.optimization_barrier(jnp.mean(jnp.square(values - average), axis=-1, keepdims=True))
    return (values - average) * lax.rsqrt(spread + epsilon) * gain + bias

def one_crop(crop_rep, crop_mask, amax_history, in_gain, in_bias, proj_weight, gate_weight, out_gain, out_bias, out_weight):
    normed = layer_norm(crop_rep.astype(jnp.float32), in_gain, in_bias).astype(jnp.bfloat16)
    flat = normed.reshape(N * N, C)
    masking = crop_mask.astype(jnp.float32).reshape(N * N, 1)

    def project(which):
        return jnp.dot(flat, proj_weight[:, which, :], preferred_element_type=jnp.float32)
    left_proj = masking * jax.nn.sigmoid(project(1)) * project(0)
    right_proj = masking * jax.nn.sigmoid(project(3)) * project(2)
    crop_amax = jnp.stack([lax.optimization_barrier(jnp.max(jnp.abs(left_proj), axis=0)), lax.optimization_barrier(jnp.max(jnp.abs(right_proj), axis=0))])
    scales = amax_history / format_limit
    left_q = jnp.clip(left_proj / scales[0], -format_limit, format_limit).astype(jnp.bfloat16).reshape(N, N, C)
    right_q = jnp.clip(right_proj / scales[1], -format_limit, format_limit).astype(jnp.bfloat16).reshape(N, N, C)
    products = jnp.einsum('ikc,jkc->ijc', left_q.astype(jnp.float32), right_q.astype(jnp.float32))
    triangle = (products * (scales[0] * scales[1])).astype(jnp.bfloat16)
    tnorm = layer_norm(triangle.astype(jnp.float32), out_gain, out_bias).astype(jnp.bfloat16)
    gating = jax.nn.sigmoid(jnp.dot(flat, gate_weight, preferred_element_type=jnp.float32))
    mixing = jnp.dot(tnorm.reshape(N * N, C), out_weight, preferred_element_type=jnp.float32)
    update = (gating * mixing).astype(jnp.bfloat16).reshape(N, N, C)
    return (update, crop_amax)

def reference(pair_rep, pair_mask, amax_history, in_gain, in_bias, proj_weight, gate_weight, out_gain, out_bias, out_weight):
    updates = []
    maxima = []
    for crop in range(CROPS):
        update, crop_amax = one_crop(pair_rep[crop], pair_mask[crop], amax_history, in_gain, in_bias, proj_weight, gate_weight, out_gain, out_bias, out_weight)
        updates.append(update)
        maxima.append(crop_amax)
    new_amax = maxima[0]
    for crop_amax in maxima[1:]:
        new_amax = jnp.maximum(new_amax, crop_amax)
    return (jnp.stack(updates), new_amax)
```

```python
import functools

import jax
import jax.numpy as jnp
from jax import lax
from jax.experimental import pallas as pl
from jax.experimental.pallas import tpu as pltpu
from jax.sharding import PartitionSpec as P

epsilon = 1e-05
format_limit = 448.0
LANES = 128
f32, bf16 = jnp.float32, jnp.bfloat16
MESH = pl.DeviceIdType.MESH


def kernel(
    dims,
    rep_ref,
    mask_ref,
    hist_ref,
    hist_smem,
    in_gain_ref,
    in_bias_ref,
    proj_ref,
    gate_ref,
    out_gain_smem,
    out_bias_smem,
    out_weight_ref,
    out_ref,
    amax_ref,
    normed,
    maskf,
    inverse,
    peak,
    left_s,
    right_s,
    left_b,
    left_t,
    left_r,
    left_e,
    right_all,
    own_t,
    send_t,
    recv_t,
    ret_t,
    full_t,
    spread_t,
    mix_w,
    ow_pad,
    vecs,
    gating,
    peaks,
    peak_send,
    peak_recv,
    z_send,
    z_recv,
    l_send,
    l_recv,
    x_send,
    x_recv,
    c_send,
    c_recv,
    e_send,
    e_recv,
):
    nz, ny, rows, cols, half, chunks = dims
    ratio = nz // ny
    channels = 2 * half
    per = LANES // rows
    pairs = -(-half // (2 * per))
    groups = 2 * pairs
    span = per * rows
    slot = LANES // (2 * ratio)
    z, y, col = lax.axis_index("gx"), lax.axis_index("gy"), lax.axis_index("col")
    members = nz * ny
    me = z * ny + y
    is_end = (z == 0) | (z == nz - 1)
    is_next = (z == 1) | (z == nz - 2)
    high_side = 2 * z >= nz
    sgn = jnp.where(high_side, 1, -1)
    end = jnp.where(high_side, nz - 1, 0)
    inward = jnp.where(high_side, 1, 0)
    up_ok = z <= nz - 3
    down_ok = z >= 2
    unroll = max(u for u in range(1, 9) if rows % u == 0)

    barrier = pltpu.get_barrier_semaphore()

    def greet(t, carry):
        peer = lax.rem(me + t, members)
        pl.semaphore_signal(
            barrier, inc=1, device_id={"gx": peer // ny, "gy": lax.rem(peer, ny)}, device_id_type=MESH
        )
        return carry

    lax.fori_loop(1, members, greet, 0)
    pl.semaphore_signal(barrier, inc=1, device_id={"col": 1 - col}, device_id_type=MESH)

    @pl.when(is_end)
    def _():
        pl.semaphore_signal(
            barrier, inc=1, device_id={"gx": z - sgn, "col": 1 - col}, device_id_type=MESH
        )

    normed[pl.ds(rows * cols, LANES), :] = jnp.zeros((LANES, channels), bf16)
    step_rows = unroll

    def norm_step(b, carry):
        values = rep_ref[pl.ds(b * step_rows, step_rows)].reshape(step_rows * cols, channels).astype(f32)
        average = jnp.mean(values, axis=-1, keepdims=True)
        centred = values - average
        var = jnp.mean(jnp.square(centred), axis=-1, keepdims=True)
        result = centred * lax.rsqrt(var + epsilon) * in_gain_ref[...] + in_bias_ref[...]
        start = pl.multiple_of(b * step_rows * cols, 16)
        normed[pl.ds(start, step_rows * cols), :] = result.astype(bf16)
        return carry

    lax.fori_loop(0, rows // step_rows, norm_step, 0)
    maskf[...] = jnp.zeros_like(maskf)
    maskf[:, 0:cols] = mask_ref[...].astype(f32)
    scaled = format_limit / hist_ref[...]
    flipped = jnp.concatenate([scaled[0:1], scaled[1:2]], axis=1)
    flipped = jnp.broadcast_to(flipped, (channels, channels))
    inverse[...] = jnp.transpose(flipped)
    peak[...] = jnp.zeros_like(peak)
    tail = left_s.shape[0] - half * rows
    left_s[pl.ds(half * rows, tail), :] = jnp.zeros((tail, LANES), f32)
    right_s[pl.ds(half * rows, tail), :] = jnp.zeros((tail, LANES), f32)

    def project(side, target):
        base = side * half

        def one(i):
            block = normed[pl.ds(pl.multiple_of(i * cols, 16), LANES), :]
            p = lax.dot_general(
                proj_ref[2 * base : 2 * base + channels, :],
                block,
                (((1,), (1,)), ((), ())),
                preferred_element_type=f32,
            )
            value = jax.nn.sigmoid(p[half:]) * p[:half] * maskf[pl.ds(i, 1), :]
            target[pl.ds(i, half, stride=rows), :] = jnp.clip(
                value * inverse[base : base + half, :], -format_limit, format_limit
            )
            return jnp.abs(value)

        def step(b, top):
            for u in range(unroll):
                top = jnp.maximum(top, one(b * unroll + u))
            return top

        top = lax.fori_loop(0, rows // unroll, step, jnp.zeros((half, LANES), f32))
        peak[base : base + half, :] = top

    project(1, right_s)
    bounds = [pairs * c // chunks for c in range(chunks + 1)]

    def z_copy(source, c, direction):
        window = pl.ds(2 * bounds[c], 2 * (bounds[c + 1] - bounds[c]))
        toward = z + 1 - 2 * direction
        return pltpu.make_async_remote_copy(
            src_ref=right_all.at[source, window],
            dst_ref=right_all.at[source, window],
            send_sem=z_send.at[direction, source, c],
            recv_sem=z_recv.at[source, c],
            device_id={"gx": toward},
            device_id_type=MESH,
        )

    def left_copy(c):
        window = pl.ds(2 * bounds[c], 2 * (bounds[c + 1] - bounds[c]))
        return pltpu.make_async_remote_copy(
            src_ref=left_t.at[window],
            dst_ref=left_r.at[window],
            send_sem=l_send.at[c],
            recv_sem=l_recv.at[c],
            device_id={"gx": z - sgn},
            device_id_type=MESH,
        )

    pl.semaphore_wait(barrier, members + jnp.where(is_next, 1, 0))
    early = chunks // 2
    for c in range(chunks):
        for g in range(2 * bounds[c], 2 * bounds[c + 1]):
            tile = jnp.transpose(right_s[g * span : g * span + LANES, :])
            right_all[z, g] = tile[:cols].astype(bf16)
        now = True if c < early else jnp.logical_not(is_end)

        @pl.when(up_ok & now)
        def _():
            z_copy(z, c, 0).start()

        @pl.when(down_ok & now)
        def _():
            z_copy(z, c, 1).start()

    project(0, left_s)

    @pl.when(is_end)
    def _():
        for c in range(chunks):
            for g in range(2 * bounds[c], 2 * bounds[c + 1]):
                tile = jnp.transpose(left_s[g * span : g * span + LANES, :])
                left_t[g] = tile[:cols].astype(bf16)
            if c >= early:
                z_copy(z, c, inward).start()
            left_copy(c).start()

    for g in range(groups):
        left_b[g] = left_s[g * span : g * span + LANES, :].astype(bf16)

    peaks[me] = jnp.broadcast_to(jnp.max(jnp.transpose(peak[...]), axis=0, keepdims=True), (8, channels))

    def spread_peak(t, carry):
        peer = lax.rem(me + t, members)
        pltpu.make_async_remote_copy(
            src_ref=peaks.at[me],
            dst_ref=peaks.at[me],
            send_sem=peak_send,
            recv_sem=peak_recv,
            device_id={"gx": peer // ny, "gy": lax.rem(peer, ny)},
            device_id_type=MESH,
        ).start()
        return carry

    lax.fori_loop(1, members, spread_peak, 0)

    lane = lax.broadcasted_iota(jnp.int32, (rows, LANES), 1)

    def triangle_pair(lhs, r, p):
        halves = []
        for u in range(2):
            res = lax.dot_general(
                lhs[2 * p + u][:, :cols],
                right_all[r, 2 * p + u],
                (((1,), (0,)), ((), ())),
                preferred_element_type=f32,
            )
            t = res[:rows]
            for s in range(1, per):
                t = jnp.where(lane >= s * rows, res[s * rows : (s + 1) * rows], t)
            halves.append(t)
        return jnp.concatenate(halves, axis=0)

    def x_copy(rowset, target, sub, c, source):
        window = pl.ds(bounds[c], bounds[c + 1] - bounds[c])
        return pltpu.make_async_remote_copy(
            src_ref=send_t.at[rowset, target, sub, window],
            dst_ref=recv_t.at[rowset, source, sub, window],
            send_sem=x_send.at[rowset, target, sub, c],
            recv_sem=x_recv.at[rowset, source, sub, c],
            device_id={"gy": target},
            device_id_type=MESH,
        )

    def triangle_block(rowset, r, c):
        owner, sub = r // ratio, lax.rem(r, ratio)
        slot = jnp.where(owner == y, sub, ratio)
        lhs = left_e if rowset else left_b
        for p in range(bounds[c], bounds[c + 1]):
            t = triangle_pair(lhs, r, p)
            own_t[rowset, slot, p] = t
            send_t[rowset, owner, sub, p] = t.astype(bf16)

        @pl.when(owner != y)
        def _():
            x_copy(rowset, owner, sub, c, y).start()

    for c in range(chunks):
        triangle_block(0, z, c)

    def gate_step(b, carry):
        for u in range(unroll):
            i = b * unroll + u
            block = normed[pl.ds(pl.multiple_of(i * cols, 16), LANES), :]
            gating[i] = jax.nn.sigmoid(
                lax.dot_general(
                    gate_ref[...], block, (((1,), (1,)), ((), ())), preferred_element_type=f32
                )
            )
        return carry

    lax.fori_loop(0, rows // unroll, gate_step, 0)
    ow_pad[...] = jnp.zeros_like(ow_pad)
    stretch = ow_pad.shape[0] // 2
    square = jnp.concatenate(
        [out_weight_ref[...].astype(f32), jnp.zeros((LANES - half, channels), f32)], axis=0
    )
    turned = jnp.transpose(square)
    for cc in range(2):
        ow_pad[cc * stretch : cc * stretch + half, :] = turned[cc * half : (cc + 1) * half, :]
    for s in range(per):
        parts = [ow_pad[pl.ds(cc * stretch + s, slot, stride=per), :] for cc in range(2)]
        parts.append(jnp.zeros((LANES - 2 * slot, LANES), f32))
        back = jnp.transpose(jnp.concatenate(parts, axis=0))
        mix_w[s * half : (s + 1) * half, :] = back[:half].astype(bf16)
    spread_t[...] = jnp.zeros_like(spread_t)

    group_lane = lax.broadcasted_iota(jnp.int32, (1, LANES), 1)

    def lane_vector(scalar_of, g):
        ch = [jnp.minimum(g * per + s, half - 1) for s in range(per)]
        vector = jnp.full((1, LANES), scalar_of(ch[0]), f32)
        for s in range(1, per):
            vector = jnp.where(group_lane >= s * rows, scalar_of(ch[s]), vector)
        return vector

    def scale_of(ch):
        return (hist_smem[0, ch] / format_limit) * (hist_smem[1, ch] / format_limit)

    def fill_vectors(g, carry):
        vecs[0, pl.ds(g, 1), :] = lane_vector(scale_of, g)
        for cc in range(2):
            vecs[1 + cc, pl.ds(g, 1), :] = lane_vector(lambda ch: out_gain_smem[cc * half + ch], g)
            vecs[3 + cc, pl.ds(g, 1), :] = lane_vector(lambda ch: out_bias_smem[cc * half + ch], g)
        return carry

    lax.fori_loop(0, groups, fill_vectors, 0)

    def pair_vector(v, p):
        parts = [jnp.broadcast_to(vecs[v, 2 * p + u : 2 * p + u + 1, :], (rows, LANES)) for u in range(2)]
        return jnp.concatenate(parts, axis=0)

    def c_copy(sub, c):
        window = pl.ds(bounds[c], bounds[c + 1] - bounds[c])
        return pltpu.make_async_remote_copy(
            src_ref=full_t.at[col, sub, window],
            dst_ref=full_t.at[col, sub, window],
            send_sem=c_send.at[sub, c],
            recv_sem=c_recv.at[sub, c],
            device_id={"col": 1 - col},
            device_id_type=MESH,
        )

    def end_copy(sub, c, source, target):
        window = pl.ds(bounds[c], bounds[c + 1] - bounds[c])
        return pltpu.make_async_remote_copy(
            src_ref=ret_t.at[sub, window],
            dst_ref=full_t.at[source, sub, window],
            send_sem=e_send.at[target, sub, c],
            recv_sem=e_recv.at[source, sub, c],
            device_id={"gx": end, "col": target},
            device_id_type=MESH,
        )

    def finish_block(rowset, r, c):
        owner, sub = r // ratio, lax.rem(r, ratio)

        @pl.when(owner == y)
        def _():
            def arrive(t, carry):
                x_copy(rowset, y, sub, c, lax.rem(y + t, ny)).wait_recv()
                return carry

            lax.fori_loop(1, ny, arrive, 0)
            for p in range(bounds[c], bounds[c + 1]):
                total = own_t[rowset, sub, p]
                for t in range(1, ny):
                    total = total + recv_t[rowset, lax.rem(y + t, ny), sub, p].astype(f32)
                result = (total * pair_vector(0, p)).astype(bf16)
                if rowset:
                    ret_t[sub, p] = result
                else:
                    full_t[col, sub, p] = result
            if rowset:
                end_copy(sub, c, col, col).start()
                end_copy(sub, c, col, 1 - col).start()
            else:
                c_copy(sub, c).start()

    for c in range(chunks):
        finish_block(0, z, c)

    row_at = lax.broadcasted_iota(jnp.int32, (2 * rows, LANES), 0) // rows
    lane_at = lax.broadcasted_iota(jnp.int32, (2 * rows, LANES), 1) // rows
    valid = (((pairs - 1) * 2 + row_at) * per + lane_at) < half

    def segment_mean(pair_sum):
        x = pair_sum[:rows] + pair_sum[rows:]
        total = x
        for s in range(1, per):
            total = total + pltpu.roll(x, s * rows, 1)
        result = total
        for s in range(1, per):
            moved = pltpu.roll(total, LANES - s * rows, 1)
            result = jnp.where(lane < (per - s) * rows, moved, result)
        result = result * (1.0 / channels)
        return jnp.concatenate([result, result], axis=0)

    def norm_sub(sub):
        r = y * ratio + sub
        returned = is_end & (r != z)

        @pl.when(returned)
        def _():
            for c in range(chunks):
                for cc in range(2):
                    end_copy(sub, c, cc, col).wait_recv()

        @pl.when(jnp.logical_not(returned))
        def _():
            for c in range(chunks):
                c_copy(sub, c).wait_recv()

        total = jnp.zeros((2 * rows, LANES), f32)
        for p in range(pairs):
            total = total + full_t[0, sub, p].astype(f32) + full_t[1, sub, p].astype(f32)
        mean = segment_mean(total)
        squares = jnp.zeros((2 * rows, LANES), f32)
        for p in range(pairs):
            for cc in range(2):
                square = jnp.square(full_t[cc, sub, p].astype(f32) - mean)
                if p == pairs - 1:
                    square = jnp.where(valid, square, 0.0)
                squares = squares + square
        factor = lax.rsqrt(segment_mean(squares) + epsilon)
        for p in range(pairs):
            for cc in range(2):
                t = (full_t[cc, sub, p].astype(f32) - mean) * factor
                t = t * pair_vector(1 + cc, p) + pair_vector(3 + cc, p)
                for u in range(2):
                    at = (sub * 2 + cc) * slot + 2 * p + u
                    spread_t[pl.ds(at, rows, stride=LANES), :] = t[u * rows : (u + 1) * rows]

    first_low = jnp.logical_xor(2 * y < ny, is_end)
    order = jnp.where(first_low, ratio - 1, 0)
    step_sign = jnp.where(first_low, -1, 1)

    end_sequence = [("right", c) for c in range(early)] + [("left", c) for c in range(early)]
    for c in range(early, chunks):
        end_sequence += [("right", c), ("left", c)]
    within = nz == 4 and ratio == 2

    @pl.when(is_next)
    def _():
        lefts, held, pending = [], [], []
        for s in range(2 * chunks):
            kind, ce = end_sequence[s]
            k, c = 1 + s // chunks, s % chunks
            source = z - sgn * k
            todo = []
            if kind == "right":
                z_copy(end, ce, inward).wait_recv()
                z_copy(end, ce, inward).start()
            if within and s == 2 * chunks - 1:
                norm_sub(order)
            z_copy(source, c, 1 - inward).wait_recv()
            if kind == "left":
                left_copy(ce).wait_recv()
                for g in range(2 * bounds[ce], 2 * bounds[ce + 1]):
                    tile = jnp.concatenate(
                        [left_r[g].astype(f32), jnp.zeros((LANES - cols, LANES), f32)], axis=0
                    )
                    left_e[g] = jnp.transpose(tile).astype(bf16)
                lefts.append(ce)
            if c in lefts:
                todo.append((1, source, c))
            todo.append((0, source, c))
            if kind == "left":
                todo += [(1, z - sgn * kk, ce) for kk, cc in held if cc == ce]
                todo.append((1, z, ce))
            else:
                todo.append((0, end, ce))
            held.append((k, c))
            for block in todo:
                triangle_block(*block)
            for block in pending:
                finish_block(*block)
            pending = todo
        for block in pending:
            finish_block(*block)

        def farther(k, carry):
            for c in range(chunks):
                z_copy(z - sgn * k, c, 1 - inward).wait_recv()
                for rowset in (1, 0):
                    triangle_block(rowset, z - sgn * k, c)
                for rowset in (1, 0):
                    finish_block(rowset, z - sgn * k, c)
            return carry

        if nz > 4:
            lax.fori_loop(3, nz - 1, farther, 0)

    if nz > 4:

        @pl.when(jnp.logical_not(is_end | is_next))
        def _():
            def ring_step(d, carry):
                for c in range(chunks):
                    for source, direction, there in ((z - d, 0, z - d >= 0), (z + d, 1, z + d < nz)):

                        @pl.when(there)
                        def _(source=source, direction=direction, c=c):
                            z_copy(source, c, direction).wait_recv()
                            z_copy(source, c, direction).start()
                            triangle_block(0, source, c)
                            finish_block(0, source, c)

                return carry

            lax.fori_loop(1, nz - 1, ring_step, 0)

    if within:

        @pl.when(is_end)
        def _():
            norm_sub(order)

        norm_sub(order + step_sign)
    else:
        for t in range(ratio):
            norm_sub(order + step_sign * t)

    wide = lax.broadcasted_iota(jnp.int32, (half, LANES), 1)

    def mix_one(i):
        start = pl.multiple_of(i * LANES, LANES)
        tile = spread_t[pl.ds(start, LANES), :].astype(bf16)
        parts = [tile[rr * 2 * slot : (rr + 1) * 2 * slot] for rr in range(ratio)]
        res = jnp.dot(
            mix_w[:, 0 : 2 * slot], jnp.concatenate(parts, axis=1), preferred_element_type=f32
        )
        mixing = None
        for rr in range(ratio):
            total = None
            for s in range(per):
                piece = res[s * half : (s + 1) * half, rr * LANES : (rr + 1) * LANES]
                shift = (rr - s) * rows % LANES
                piece = pltpu.roll(piece, shift, 1) if shift else piece
                total = piece if total is None else total + piece
            mixing = total if mixing is None else jnp.where(wide >= rr * rows, total, mixing)
        out_ref[i] = (gating[i] * mixing)[:, :cols].astype(bf16)

    def mix_step(b, carry):
        for u in range(unroll):
            mix_one(b * unroll + u)
        return carry

    lax.fori_loop(0, rows // unroll, mix_step, 0)

    others = peaks.at[pl.ds(0, members - 1)]
    pltpu.make_async_copy(others, others, peak_recv).wait()
    top = jnp.max(jnp.max(peaks[...], axis=0), axis=0, keepdims=True)
    amax_ref[0:1, :] = top[:, :half]
    amax_ref[1:2, :] = top[:, half:]

    pltpu.make_async_copy(others, others, peak_send).wait()

    for sub in range(ratio):
        r = y * ratio + sub

        @pl.when(jnp.logical_not(is_end) | (r == z))
        def _(sub=sub):
            for c in range(chunks):
                c_copy(sub, c).wait_send()

        @pl.when(is_next & (r != end))
        def _(sub=sub):
            for c in range(chunks):
                for target in range(2):
                    end_copy(sub, c, col, target).wait_send()

    def drain_x(t, carry):
        target = lax.rem(y + t, ny)
        for sub in range(ratio):
            r = target * ratio + sub

            @pl.when(jnp.logical_not(is_end) | (r == z))
            def _(sub=sub):
                for c in range(chunks):
                    x_copy(0, target, sub, c, y).wait_send()

            @pl.when(is_next & (r != end))
            def _(sub=sub):
                for c in range(chunks):
                    x_copy(1, target, sub, c, y).wait_send()

        return carry

    lax.fori_loop(1, ny, drain_x, 0)

    @pl.when(is_end)
    def _():
        for c in range(chunks):
            left_copy(c).wait_send()

    def drain_z(source, carry):
        @pl.when((source <= z) & up_ok)
        def _():
            for c in range(chunks):
                z_copy(source, c, 0).wait_send()

        @pl.when((source >= z) & down_ok)
        def _():
            for c in range(chunks):
                z_copy(source, c, 1).wait_send()

        return carry

    lax.fori_loop(0, nz, drain_z, 0)


def on_device(
    nz,
    ny,
    pair_rep,
    pair_mask,
    amax_history,
    in_gain,
    in_bias,
    proj_weight,
    gate_weight,
    out_gain,
    out_bias,
    out_weight,
):
    crops, rows, cols, channels = pair_rep.shape
    half = proj_weight.shape[2]
    chunks = 4
    ratio = nz // ny
    per = LANES // rows
    pairs = -(-half // (2 * per))
    groups = 2 * pairs
    slot = LANES // (2 * ratio)
    members = nz * ny
    weights = jnp.transpose(proj_weight, (1, 2, 0)).reshape(4 * half, channels)
    scratch_rows = -(-((groups - 1) * per * rows + LANES) // 8) * 8
    dma = pltpu.SemaphoreType.DMA
    vmem = pl.BlockSpec(memory_space=pltpu.VMEM)
    smem = pl.BlockSpec(memory_space=pltpu.SMEM)
    tile = (2 * rows, LANES)
    update, new_amax = pl.pallas_call(
        functools.partial(kernel, (nz, ny, rows, cols, half, chunks)),
        out_shape=(
            jax.ShapeDtypeStruct((rows, half, cols), bf16),
            jax.ShapeDtypeStruct((2, half), f32),
        ),
        in_specs=[vmem, vmem, vmem, smem, vmem, vmem, vmem, vmem, smem, smem, vmem],
        out_specs=(vmem, vmem),
        scratch_shapes=[
            pltpu.VMEM((rows * cols + LANES, channels), bf16),
            pltpu.VMEM((rows, LANES), f32),
            pltpu.VMEM((channels, LANES), f32),
            pltpu.VMEM((channels, LANES), f32),
            pltpu.VMEM((scratch_rows, LANES), f32),
            pltpu.VMEM((scratch_rows, LANES), f32),
            pltpu.VMEM((groups, LANES, LANES), bf16),
            pltpu.VMEM((groups, cols, LANES), bf16),
            pltpu.VMEM((groups, cols, LANES), bf16),
            pltpu.VMEM((groups, LANES, LANES), bf16),
            pltpu.VMEM((nz, groups, cols, LANES), bf16),
            pltpu.VMEM((2, ratio + 1, pairs) + tile, f32),
            pltpu.VMEM((2, ny, ratio, pairs) + tile, bf16),
            pltpu.VMEM((2, ny, ratio, pairs) + tile, bf16),
            pltpu.VMEM((ratio, pairs) + tile, bf16),
            pltpu.VMEM((2, ratio, pairs) + tile, bf16),
            pltpu.VMEM((rows * LANES, LANES), f32),
            pltpu.VMEM((per * half, LANES), bf16),
            pltpu.VMEM((2 * slot * per, LANES), f32),
            pltpu.VMEM((5, groups, LANES), f32),
            pltpu.VMEM((rows, half, LANES), f32),
            pltpu.VMEM((members, 8, channels), f32),
            dma,
            dma,
            dma((2, nz, chunks)),
            dma((nz, chunks)),
            dma((chunks,)),
            dma((chunks,)),
            dma((2, ny, ratio, chunks)),
            dma((2, ny, ratio, chunks)),
            dma((ratio, chunks)),
            dma((ratio, chunks)),
            dma((2, ratio, chunks)),
            dma((2, ratio, chunks)),
        ],
        compiler_params=pltpu.CompilerParams(
            collective_id=0, has_side_effects=True, vmem_limit_bytes=56 * 1024 * 1024
        ),
    )(
        pair_rep[0],
        pair_mask[0],
        amax_history,
        amax_history,
        in_gain.reshape(1, channels),
        in_bias.reshape(1, channels),
        weights,
        gate_weight.T,
        out_gain,
        out_bias,
        out_weight.T,
    )
    return jnp.transpose(update, (0, 2, 1))[None], new_amax


def solution(mesh):
    placed = (
        P("ga", "gx", "gy", None),
        P("ga", "gx", "gy"),
        P(None, "col"),
        P(),
        P(),
        P(None, None, "col"),
        P(None, "col"),
        P(),
        P(),
        P(None, "col"),
    )
    return jax.shard_map(
        functools.partial(on_device, mesh.shape["gx"], mesh.shape["gy"]),
        mesh=mesh,
        in_specs=placed,
        out_specs=(P("ga", "gx", "gy", "col"), P("ga", "col")),
        check_vma=False,
    )
```

```python
import functools

import jax
import jax.numpy as jnp
from jax import lax
from jax.experimental import pallas as pl
from jax.experimental.pallas import tpu as pltpu
from jax.sharding import PartitionSpec as P

epsilon = 1e-05
format_limit = 448.0
LANES = 128
f32, bf16 = jnp.float32, jnp.bfloat16
MESH = pl.DeviceIdType.MESH


def kernel(
    dims,
    rep_ref,
    mask_ref,
    hist_ref,
    hist_smem,
    in_gain_ref,
    in_bias_ref,
    proj_ref,
    gate_ref,
    out_gain_smem,
    out_bias_smem,
    out_weight_ref,
    out_hbm,
    amax_hbm,
    normed,
    maskf,
    inverse,
    peak,
    left_s,
    right_s,
    left_b,
    left_t,
    left_r,
    left_e,
    right_all,
    own_t,
    send_t,
    recv_t,
    ret_t,
    full_t,
    spread_t,
    out_ref,
    amax_ref,
    vecs,
    gating,
    peaks,
    peak_send,
    peak_recv,
    z_send,
    z_recv,
    l_send,
    l_recv,
    x_send,
    x_recv,
    c_send,
    c_recv,
    e_send,
    e_recv,
    out_sem,
    amax_sem,
):
    nz, ny, rows, cols, half, chunks = dims
    ratio = nz // ny
    channels = 2 * half
    per = LANES // rows
    pairs = -(-half // (2 * per))
    groups = 2 * pairs
    span = per * rows
    pitch = channels + 1
    z, y, col = lax.axis_index("gx"), lax.axis_index("gy"), lax.axis_index("col")
    members = nz * ny
    me = z * ny + y
    is_end = (z == 0) | (z == nz - 1)
    is_next = (z == 1) | (z == nz - 2)
    high_side = 2 * z >= nz
    sgn = jnp.where(high_side, 1, -1)
    end = jnp.where(high_side, nz - 1, 0)
    inward = jnp.where(high_side, 1, 0)
    near = z - sgn
    unroll = max(u for u in range(1, 9) if rows % u == 0)

    barrier = pltpu.get_barrier_semaphore()

    def greet(t, carry):
        peer = lax.rem(me + t, members)
        pl.semaphore_signal(
            barrier, inc=1, device_id={"gx": peer // ny, "gy": lax.rem(peer, ny)}, device_id_type=MESH
        )
        return carry

    lax.fori_loop(1, members, greet, 0)
    pl.semaphore_signal(barrier, inc=1, device_id={"col": 1 - col}, device_id_type=MESH)

    normed[pl.ds(rows * cols, LANES), :] = jnp.zeros((LANES, channels), bf16)
    step_rows = unroll

    def norm_step(b, carry):
        values = rep_ref[pl.ds(b * step_rows, step_rows)].reshape(step_rows * cols, channels).astype(f32)
        average = jnp.mean(values, axis=-1, keepdims=True)
        centred = values - average
        var = jnp.mean(jnp.square(centred), axis=-1, keepdims=True)
        result = centred * lax.rsqrt(var + epsilon) * in_gain_ref[...] + in_bias_ref[...]
        start = pl.multiple_of(b * step_rows * cols, 16)
        normed[pl.ds(start, step_rows * cols), :] = result.astype(bf16)
        return carry

    lax.fori_loop(0, rows // step_rows, norm_step, 0)
    maskf[...] = jnp.zeros_like(maskf)
    maskf[:, 0:cols] = mask_ref[...].astype(f32)
    scaled = format_limit / hist_ref[...]
    flipped = jnp.concatenate([scaled[0:1], scaled[1:2]], axis=1)
    flipped = jnp.broadcast_to(flipped, (channels, channels))
    inverse[...] = jnp.transpose(flipped)
    peak[...] = jnp.zeros_like(peak)
    tail = left_s.shape[0] - half * rows
    left_s[pl.ds(half * rows, tail), :] = jnp.zeros((tail, LANES), f32)
    right_s[pl.ds(half * rows, tail), :] = jnp.zeros((tail, LANES), f32)

    def project(side, target):
        base = side * half

        def one(i):
            block = normed[pl.ds(pl.multiple_of(i * cols, 16), LANES), :]
            p = lax.dot_general(
                proj_ref[2 * base : 2 * base + channels, :],
                block,
                (((1,), (1,)), ((), ())),
                preferred_element_type=f32,
            )
            value = jax.nn.sigmoid(p[half:]) * p[:half] * maskf[pl.ds(i, 1), :]
            target[pl.ds(i, half, stride=rows), :] = jnp.clip(
                value * inverse[base : base + half, :], -format_limit, format_limit
            )
            return jnp.abs(value)

        def step(b, top):
            for u in range(unroll):
                top = jnp.maximum(top, one(b * unroll + u))
            return top

        top = lax.fori_loop(0, rows // unroll, step, jnp.zeros((half, LANES), f32))
        peak[base : base + half, :] = top

    project(1, right_s)
    bounds = [pairs * c // chunks for c in range(chunks + 1)]

    def z_copy(source, c, direction):
        window = pl.ds(2 * bounds[c], 2 * (bounds[c + 1] - bounds[c]))
        toward = z + 1 - 2 * direction
        return pltpu.make_async_remote_copy(
            src_ref=right_all.at[source, window],
            dst_ref=right_all.at[source, window],
            send_sem=z_send.at[direction, source],
            recv_sem=z_recv.at[source, c],
            device_id={"gx": toward},
            device_id_type=MESH,
        )

    def left_copy(c):
        window = pl.ds(2 * bounds[c], 2 * (bounds[c + 1] - bounds[c]))
        return pltpu.make_async_remote_copy(
            src_ref=left_t.at[window],
            dst_ref=left_r.at[window],
            send_sem=l_send,
            recv_sem=l_recv.at[c],
            device_id={"gx": near},
            device_id_type=MESH,
        )

    pl.semaphore_wait(barrier, members)
    early = chunks // 2
    for c in range(chunks):
        for g in range(2 * bounds[c], 2 * bounds[c + 1]):
            tile = jnp.transpose(right_s[g * span : g * span + LANES, :])
            right_all[z, g] = tile[:cols].astype(bf16)
        now = True if c < early else jnp.logical_not(is_end)

        @pl.when((z < nz - 1) & now)
        def _():
            z_copy(z, c, 0).start()

        @pl.when((z > 0) & now)
        def _():
            z_copy(z, c, 1).start()

    project(0, left_s)

    @pl.when(is_end)
    def _():
        for c in range(chunks):
            for g in range(2 * bounds[c], 2 * bounds[c + 1]):
                tile = jnp.transpose(left_s[g * span : g * span + LANES, :])
                left_t[g] = tile[:cols].astype(bf16)
            if c >= early:
                z_copy(z, c, inward).start()
            left_copy(c).start()

    for g in range(groups):
        left_b[g] = left_s[g * span : g * span + LANES, :].astype(bf16)

    peaks[me] = jnp.broadcast_to(jnp.max(jnp.transpose(peak[...]), axis=0, keepdims=True), (8, channels))

    def spread_peak(t, carry):
        peer = lax.rem(me + t, members)
        pltpu.make_async_remote_copy(
            src_ref=peaks.at[me],
            dst_ref=peaks.at[me],
            send_sem=peak_send,
            recv_sem=peak_recv,
            device_id={"gx": peer // ny, "gy": lax.rem(peer, ny)},
            device_id_type=MESH,
        ).start()
        return carry

    lax.fori_loop(1, members, spread_peak, 0)

    lane = lax.broadcasted_iota(jnp.int32, (rows, LANES), 1)

    def triangle_pair(lhs, r, p):
        halves = []
        for u in range(2):
            res = lax.dot_general(
                lhs[2 * p + u][:, :cols],
                right_all[r, 2 * p + u],
                (((1,), (0,)), ((), ())),
                preferred_element_type=f32,
            )
            t = res[:rows]
            for s in range(1, per):
                t = jnp.where(lane >= s * rows, res[s * rows : (s + 1) * rows], t)
            halves.append(t)
        return jnp.concatenate(halves, axis=0)

    def x_copy(rowset, target, sub, c, source):
        window = pl.ds(bounds[c], bounds[c + 1] - bounds[c])
        return pltpu.make_async_remote_copy(
            src_ref=send_t.at[rowset, target, sub, window],
            dst_ref=recv_t.at[rowset, source, sub, window],
            send_sem=x_send.at[rowset, target, sub],
            recv_sem=x_recv.at[rowset, source, sub, c],
            device_id={"gy": target},
            device_id_type=MESH,
        )

    def triangle_block(rowset, r, c):
        owner, sub = r // ratio, lax.rem(r, ratio)
        slot = jnp.where(owner == y, sub, ratio)
        lhs = left_e if rowset else left_b
        for p in range(bounds[c], bounds[c + 1]):
            t = triangle_pair(lhs, r, p)
            own_t[rowset, slot, p] = t
            send_t[rowset, owner, sub, p] = t.astype(bf16)

        @pl.when(owner != y)
        def _():
            x_copy(rowset, owner, sub, c, y).start()

    for c in range(chunks):
        triangle_block(0, z, c)

    def gate_step(b, carry):
        for u in range(unroll):
            i = b * unroll + u
            block = normed[pl.ds(pl.multiple_of(i * cols, 16), LANES), :]
            gating[i] = jax.nn.sigmoid(
                lax.dot_general(
                    gate_ref[...], block, (((1,), (1,)), ((), ())), preferred_element_type=f32
                )
            )
        return carry

    lax.fori_loop(0, rows // unroll, gate_step, 0)
    group_lane = lax.broadcasted_iota(jnp.int32, (1, LANES), 1)

    def lane_vector(scalar_of, g):
        ch = [jnp.minimum(g * per + s, half - 1) for s in range(per)]
        vector = jnp.full((1, LANES), scalar_of(ch[0]), f32)
        for s in range(1, per):
            vector = jnp.where(group_lane >= s * rows, scalar_of(ch[s]), vector)
        return vector

    def scale_of(ch):
        return (hist_smem[0, ch] / format_limit) * (hist_smem[1, ch] / format_limit)

    def fill_vectors(g, carry):
        vecs[0, pl.ds(g, 1), :] = lane_vector(scale_of, g)
        for cc in range(2):
            vecs[1 + cc, pl.ds(g, 1), :] = lane_vector(lambda ch: out_gain_smem[cc * half + ch], g)
            vecs[3 + cc, pl.ds(g, 1), :] = lane_vector(lambda ch: out_bias_smem[cc * half + ch], g)
        return carry

    lax.fori_loop(0, groups, fill_vectors, 0)

    def pair_vector(v, p):
        parts = [jnp.broadcast_to(vecs[v, 2 * p + u : 2 * p + u + 1, :], (rows, LANES)) for u in range(2)]
        return jnp.concatenate(parts, axis=0)

    def c_copy(sub, c):
        window = pl.ds(bounds[c], bounds[c + 1] - bounds[c])
        return pltpu.make_async_remote_copy(
            src_ref=full_t.at[col, sub, window],
            dst_ref=full_t.at[col, sub, window],
            send_sem=c_send.at[sub],
            recv_sem=c_recv.at[sub, c],
            device_id={"col": 1 - col},
            device_id_type=MESH,
        )

    def end_copy(sub, c):
        window = pl.ds(bounds[c], bounds[c + 1] - bounds[c])
        return pltpu.make_async_remote_copy(
            src_ref=ret_t.at[sub, window],
            dst_ref=full_t.at[col, sub, window],
            send_sem=e_send.at[sub],
            recv_sem=e_recv.at[sub, c],
            device_id={"gx": end},
            device_id_type=MESH,
        )

    def finish_block(rowset, r, c):
        owner, sub = r // ratio, lax.rem(r, ratio)

        @pl.when(owner == y)
        def _():
            def arrive(t, carry):
                x_copy(rowset, y, sub, c, lax.rem(y + t, ny)).wait_recv()
                return carry

            lax.fori_loop(1, ny, arrive, 0)
            for p in range(bounds[c], bounds[c + 1]):
                total = own_t[rowset, sub, p]
                for t in range(1, ny):
                    total = total + recv_t[rowset, lax.rem(y + t, ny), sub, p].astype(f32)
                result = (total * pair_vector(0, p)).astype(bf16)
                if rowset:
                    ret_t[sub, p] = result
                else:
                    full_t[col, sub, p] = result
            if rowset:
                end_copy(sub, c).start()
            else:
                c_copy(sub, c).start()

    for c in range(chunks):
        finish_block(0, z, c)

    row_at = lax.broadcasted_iota(jnp.int32, (2 * rows, LANES), 0) // rows
    lane_at = lax.broadcasted_iota(jnp.int32, (2 * rows, LANES), 1) // rows
    valid = (((pairs - 1) * 2 + row_at) * per + lane_at) < half

    def segment_mean(pair_sum):
        x = pair_sum[:rows] + pair_sum[rows:]
        total = x
        for s in range(1, per):
            total = total + pltpu.roll(x, s * rows, 1)
        result = total
        for s in range(1, per):
            moved = pltpu.roll(total, LANES - s * rows, 1)
            result = jnp.where(lane < (per - s) * rows, moved, result)
        result = result * (1.0 / channels)
        return jnp.concatenate([result, result], axis=0)

    def norm_sub(sub):
        for c in range(chunks):
            c_copy(sub, c).wait_recv()
        total = jnp.zeros((2 * rows, LANES), f32)
        for p in range(pairs):
            total = total + full_t[0, sub, p].astype(f32) + full_t[1, sub, p].astype(f32)
        mean = segment_mean(total)
        squares = jnp.zeros((2 * rows, LANES), f32)
        for p in range(pairs):
            for cc in range(2):
                square = jnp.square(full_t[cc, sub, p].astype(f32) - mean)
                if p == pairs - 1:
                    square = jnp.where(valid, square, 0.0)
                squares = squares + square
        factor = lax.rsqrt(segment_mean(squares) + epsilon)
        for p in range(pairs):
            for cc in range(2):
                t = (full_t[cc, sub, p].astype(f32) - mean) * factor
                t = t * pair_vector(1 + cc, p) + pair_vector(3 + cc, p)
                for ch in range(2 * p * per, min(2 * (p + 1) * per, half)):
                    u, s = ch // per - 2 * p, ch % per
                    piece = t[u * rows : (u + 1) * rows]
                    piece = pltpu.roll(piece, LANES - s * rows, 1) if s else piece
                    at = sub * (rows * pitch) + cc * half + ch
                    spread_t[pl.ds(at, rows, stride=pitch), :] = piece

    first_low = jnp.logical_xor(2 * y < ny, is_end)
    order = jnp.where(first_low, ratio - 1, 0)
    step_sign = jnp.where(first_low, -1, 1)

    def norm_turn(turn):
        norm_sub(order + step_sign * turn)

    def return_block(r, c):
        owner, sub = r // ratio, lax.rem(r, ratio)

        @pl.when(owner == y)
        def _():
            end_copy(sub, c).wait_recv()
            c_copy(sub, c).start()

    end_sequence = [("right", c) for c in range(early)] + [("left", c) for c in range(early)]
    for c in range(early, chunks):
        end_sequence += [("right", c), ("left", c)]
    within = nz == 4 and ratio == 2
    returns, held, lefts = [], [], []
    for s in range(2 * chunks):
        kind, ce = end_sequence[s]
        k, c = 1 + s // chunks, s % chunks
        if kind == "left":
            lefts.append(ce)
        if c in lefts:
            returns.append((k, c))
        if kind == "left":
            returns += [(kk, ce) for kk, cc in held if cc == ce]
        held.append((k, c))

    @pl.when(is_next)
    def _():
        lefts, held, pending = [], [], []
        for s in range(2 * chunks):
            kind, ce = end_sequence[s]
            k, c = 1 + s // chunks, s % chunks
            source = z - sgn * k
            todo = []
            if kind == "right":
                z_copy(end, ce, inward).wait_recv()
                z_copy(end, ce, inward).start()
            if within and s == 2 * chunks - 1:
                norm_turn(0)
            z_copy(source, c, 1 - inward).wait_recv()
            if kind == "left":
                left_copy(ce).wait_recv()
                for g in range(2 * bounds[ce], 2 * bounds[ce + 1]):
                    tile = jnp.concatenate(
                        [left_r[g].astype(f32), jnp.zeros((LANES - cols, LANES), f32)], axis=0
                    )
                    left_e[g] = jnp.transpose(tile).astype(bf16)
                lefts.append(ce)
            if c in lefts:
                todo.append((1, source, c))
            todo.append((0, source, c))
            if kind == "left":
                todo += [(1, z - sgn * kk, ce) for kk, cc in held if cc == ce]
            else:
                todo.append((0, end, ce))
            held.append((k, c))
            for block in todo:
                triangle_block(*block)
            for block in pending:
                finish_block(*block)
            pending = todo
        for block in pending:
            finish_block(*block)

        def farther(k, carry):
            for c in range(chunks):
                z_copy(z - sgn * k, c, 1 - inward).wait_recv()
                for rowset in (1, 0):
                    triangle_block(rowset, z - sgn * k, c)
                for rowset in (1, 0):
                    finish_block(rowset, z - sgn * k, c)
            return carry

        if nz > 4:
            lax.fori_loop(3, nz - 1, farther, 0)

    if nz > 4:

        @pl.when(jnp.logical_not(is_end | is_next))
        def _():
            def ring_step(d, carry):
                for c in range(chunks):
                    for source, direction, there in ((z - d, 0, z - d >= 0), (z + d, 1, z + d < nz)):

                        @pl.when(there)
                        def _(source=source, direction=direction, c=c):
                            z_copy(source, c, direction).wait_recv()
                            z_copy(source, c, direction).start()
                            triangle_block(0, source, c)
                            finish_block(0, source, c)

                return carry

            lax.fori_loop(1, nz - 1, ring_step, 0)

    @pl.when(is_end)
    def _():
        for c in range(chunks):
            z_copy(near, c, 1 - inward).wait_recv()
            triangle_block(0, near, c)
            if c:
                finish_block(0, near, c - 1)
        finish_block(0, near, chunks - 1)
        if within:

            @pl.when((z // ratio == y))
            def _():
                norm_turn(0)

        for k, c in returns:
            return_block(near - sgn * k, c)

        def farther_back(k, carry):
            for c in range(chunks):
                return_block(near - sgn * k, c)
            return carry

        if nz > 4:
            lax.fori_loop(3, nz - 1, farther_back, 0)
        if within:

            @pl.when((z // ratio != y))
            def _():
                norm_turn(0)

    for turn in range(1 if within else 0, ratio):
        norm_turn(turn)

    others = peaks.at[pl.ds(0, members - 1)]
    pltpu.make_async_copy(others, others, peak_recv).wait()
    top = jnp.max(jnp.max(peaks[...], axis=0), axis=0, keepdims=True)
    amax_ref[0:1, :] = top[:, :half]
    amax_ref[1:2, :] = top[:, half:]
    pltpu.make_async_copy(amax_ref, amax_hbm, amax_sem).start()

    wide = lax.broadcasted_iota(jnp.int32, (half, LANES), 1)

    def mix_step(b, carry):
        for u in range(unroll):
            i = b * unroll + u
            tiles = [
                spread_t[pl.ds((sub * rows + i) * pitch, channels), :].astype(bf16)
                for sub in range(ratio)
            ]
            res = jnp.dot(
                out_weight_ref[...], jnp.concatenate(tiles, axis=1), preferred_element_type=f32
            )
            mixing = res[:, :LANES]
            for sub in range(1, ratio):
                part = pltpu.roll(res[:, sub * LANES : (sub + 1) * LANES], sub * rows, 1)
                mixing = jnp.where(wide >= sub * rows, part, mixing)
            out_ref[i] = (gating[i] * mixing)[:, :cols].astype(bf16)
        window = pl.ds(b * unroll, unroll)
        pltpu.make_async_copy(out_ref.at[window], out_hbm.at[window], out_sem).start()
        return carry

    lax.fori_loop(0, rows // unroll, mix_step, 0)

    pltpu.make_async_copy(others, others, peak_send).wait()

    def sent(ref, sem):
        pltpu.make_async_copy(ref, ref, sem).wait()

    for sub in range(ratio):
        r = y * ratio + sub
        sent(full_t.at[col, sub], c_send.at[sub])

        @pl.when(is_next & (r != end) & (r != z))
        def _(sub=sub):
            sent(ret_t.at[sub], e_send.at[sub])

    def drain_x(t, carry):
        target = lax.rem(y + t, ny)
        for sub in range(ratio):
            r = target * ratio + sub

            @pl.when(jnp.logical_not(is_end) | (r == z) | (r == near))
            def _(sub=sub):
                sent(send_t.at[0, target, sub], x_send.at[0, target, sub])

            @pl.when(is_next & (r != end) & (r != z))
            def _(sub=sub):
                sent(send_t.at[1, target, sub], x_send.at[1, target, sub])

        return carry

    lax.fori_loop(1, ny, drain_x, 0)

    @pl.when(is_end)
    def _():
        sent(left_t, l_send)

    def drain_z(source, carry):
        @pl.when((source <= z) & (z < nz - 1) & ((source == z) | (z <= nz - 3)))
        def _():
            sent(right_all.at[source], z_send.at[0, source])

        @pl.when((source >= z) & (z > 0) & ((source == z) | (z >= 2)))
        def _():
            sent(right_all.at[source], z_send.at[1, source])

        return carry

    lax.fori_loop(0, nz, drain_z, 0)
    pltpu.make_async_copy(amax_ref, amax_hbm, amax_sem).wait()
    pltpu.make_async_copy(out_ref, out_hbm, out_sem).wait()


def on_device(
    nz,
    ny,
    pair_rep,
    pair_mask,
    amax_history,
    in_gain,
    in_bias,
    proj_weight,
    gate_weight,
    out_gain,
    out_bias,
    out_weight,
):
    crops, rows, cols, channels = pair_rep.shape
    half = proj_weight.shape[2]
    chunks = 4
    ratio = nz // ny
    per = LANES // rows
    pairs = -(-half // (2 * per))
    groups = 2 * pairs
    members = nz * ny
    weights = jnp.transpose(proj_weight, (1, 2, 0)).reshape(4 * half, channels)
    scratch_rows = -(-((groups - 1) * per * rows + LANES) // 8) * 8
    dma = pltpu.SemaphoreType.DMA
    vmem = pl.BlockSpec(memory_space=pltpu.VMEM)
    smem = pl.BlockSpec(memory_space=pltpu.SMEM)
    hbm = pl.BlockSpec(memory_space=pl.ANY)
    tile = (2 * rows, LANES)
    update, new_amax = pl.pallas_call(
        functools.partial(kernel, (nz, ny, rows, cols, half, chunks)),
        out_shape=(
            jax.ShapeDtypeStruct((rows, half, cols), bf16),
            jax.ShapeDtypeStruct((2, half), f32),
        ),
        in_specs=[vmem, vmem, vmem, smem, vmem, vmem, vmem, vmem, smem, smem, vmem],
        out_specs=(hbm, hbm),
        scratch_shapes=[
            pltpu.VMEM((rows * cols + LANES, channels), bf16),
            pltpu.VMEM((rows, LANES), f32),
            pltpu.VMEM((channels, LANES), f32),
            pltpu.VMEM((channels, LANES), f32),
            pltpu.VMEM((scratch_rows, LANES), f32),
            pltpu.VMEM((scratch_rows, LANES), f32),
            pltpu.VMEM((groups, LANES, LANES), bf16),
            pltpu.VMEM((groups, cols, LANES), bf16),
            pltpu.VMEM((groups, cols, LANES), bf16),
            pltpu.VMEM((groups, LANES, LANES), bf16),
            pltpu.VMEM((nz, groups, cols, LANES), bf16),
            pltpu.VMEM((2, ratio + 1, pairs) + tile, f32),
            pltpu.VMEM((2, ny, ratio, pairs) + tile, bf16),
            pltpu.VMEM((2, ny, ratio, pairs) + tile, bf16),
            pltpu.VMEM((ratio, pairs) + tile, bf16),
            pltpu.VMEM((2, ratio, pairs) + tile, bf16),
            pltpu.VMEM((ratio * rows * (channels + 1) + 8, LANES), f32),
            pltpu.VMEM((rows, half, cols), bf16),
            pltpu.VMEM((2, half), f32),
            pltpu.VMEM((5, groups, LANES), f32),
            pltpu.VMEM((rows, half, LANES), f32),
            pltpu.VMEM((members, 8, channels), f32),
            dma,
            dma,
            dma((2, nz)),
            dma((nz, chunks)),
            dma,
            dma((chunks,)),
            dma((2, ny, ratio)),
            dma((2, ny, ratio, chunks)),
            dma((ratio,)),
            dma((ratio, chunks)),
            dma((ratio,)),
            dma((ratio, chunks)),
            dma,
            dma,
        ],
        compiler_params=pltpu.CompilerParams(
            collective_id=0, has_side_effects=True, vmem_limit_bytes=56 * 1024 * 1024
        ),
    )(
        pair_rep[0],
        pair_mask[0],
        amax_history,
        amax_history,
        in_gain.reshape(1, channels),
        in_bias.reshape(1, channels),
        weights,
        gate_weight.T,
        out_gain,
        out_bias,
        out_weight.T,
    )
    return jnp.transpose(update, (0, 2, 1))[None], new_amax


def solution(mesh):
    placed = (
        P("ga", "gx", "gy", None),
        P("ga", "gx", "gy"),
        P(None, "col"),
        P(),
        P(),
        P(None, None, "col"),
        P(None, "col"),
        P(),
        P(),
        P(None, "col"),
    )
    return jax.shard_map(
        functools.partial(on_device, mesh.shape["gx"], mesh.shape["gy"]),
        mesh=mesh,
        in_specs=placed,
        out_specs=(P("ga", "gx", "gy", "col"), P("ga", "col")),
        check_vma=False,
    )
```

```python
import functools

import jax
import jax.numpy as jnp
from jax import lax
from jax.experimental import pallas as pl
from jax.experimental.pallas import tpu as pltpu
from jax.sharding import PartitionSpec as P

epsilon = 1e-05
format_limit = 448.0
LANES = 128
f32, bf16 = jnp.float32, jnp.bfloat16
MESH = pl.DeviceIdType.MESH


def kernel(
    dims,
    rep_ref,
    mask_ref,
    hist_ref,
    hist_smem,
    in_gain_ref,
    in_bias_ref,
    proj_ref,
    gate_ref,
    out_gain_smem,
    out_bias_smem,
    out_weight_ref,
    out_hbm,
    amax_hbm,
    normed,
    maskf,
    inverse,
    peak,
    left_s,
    right_s,
    left_b,
    left_t,
    left_r,
    left_e,
    right_all,
    own_t,
    send_t,
    recv_t,
    ret_t,
    full_t,
    spread_t,
    out_ref,
    amax_ref,
    vecs,
    gating,
    peaks,
    peak_send,
    peak_recv,
    z_send,
    z_recv,
    l_send,
    l_recv,
    x_send,
    x_recv,
    c_send,
    c_recv,
    e_send,
    e_recv,
    out_sem,
    amax_sem,
):
    nz, ny, rows, cols, half, chunks = dims
    ratio = nz // ny
    channels = 2 * half
    per = LANES // rows
    pairs = -(-half // (2 * per))
    groups = 2 * pairs
    span = per * rows
    pitch = channels + 1
    z, y, col = lax.axis_index("gx"), lax.axis_index("gy"), lax.axis_index("col")
    members = nz * ny
    me = z * ny + y
    is_end = (z == 0) | (z == nz - 1)
    is_next = (z == 1) | (z == nz - 2)
    high_side = 2 * z >= nz
    sgn = jnp.where(high_side, 1, -1)
    end = jnp.where(high_side, nz - 1, 0)
    inward = jnp.where(high_side, 1, 0)
    near = z - sgn
    unroll = max(u for u in range(1, 9) if rows % u == 0)

    barrier = pltpu.get_barrier_semaphore()

    def greet(t, carry):
        peer = lax.rem(me + t, members)
        pl.semaphore_signal(
            barrier, inc=1, device_id={"gx": peer // ny, "gy": lax.rem(peer, ny)}, device_id_type=MESH
        )
        return carry

    lax.fori_loop(1, members, greet, 0)
    pl.semaphore_signal(barrier, inc=1, device_id={"col": 1 - col}, device_id_type=MESH)

    normed[pl.ds(rows * cols, LANES), :] = jnp.zeros((LANES, channels), bf16)
    step_rows = unroll

    def norm_step(b, carry):
        values = rep_ref[pl.ds(b * step_rows, step_rows)].reshape(step_rows * cols, channels).astype(f32)
        average = jnp.mean(values, axis=-1, keepdims=True)
        centred = values - average
        var = jnp.mean(jnp.square(centred), axis=-1, keepdims=True)
        result = centred * lax.rsqrt(var + epsilon) * in_gain_ref[...] + in_bias_ref[...]
        start = pl.multiple_of(b * step_rows * cols, 16)
        normed[pl.ds(start, step_rows * cols), :] = result.astype(bf16)
        return carry

    lax.fori_loop(0, rows // step_rows, norm_step, 0)
    maskf[...] = jnp.zeros_like(maskf)
    maskf[:, 0:cols] = mask_ref[...].astype(f32)
    scaled = format_limit / hist_ref[...]
    flipped = jnp.concatenate([scaled[0:1], scaled[1:2]], axis=1)
    flipped = jnp.broadcast_to(flipped, (channels, channels))
    inverse[...] = jnp.transpose(flipped)
    peak[...] = jnp.zeros_like(peak)
    tail = left_s.shape[0] - half * rows
    left_s[pl.ds(half * rows, tail), :] = jnp.zeros((tail, LANES), f32)
    right_s[pl.ds(half * rows, tail), :] = jnp.zeros((tail, LANES), f32)

    def project(side, target):
        base = side * half

        def one(i):
            block = normed[pl.ds(pl.multiple_of(i * cols, 16), LANES), :]
            p = lax.dot_general(
                proj_ref[2 * base : 2 * base + channels, :],
                block,
                (((1,), (1,)), ((), ())),
                preferred_element_type=f32,
            )
            value = jax.nn.sigmoid(p[half:]) * p[:half] * maskf[pl.ds(i, 1), :]
            target[pl.ds(i, half, stride=rows), :] = jnp.clip(
                value * inverse[base : base + half, :], -format_limit, format_limit
            )
            return jnp.abs(value)

        def step(b, top):
            for u in range(unroll):
                top = jnp.maximum(top, one(b * unroll + u))
            return top

        top = lax.fori_loop(0, rows // unroll, step, jnp.zeros((half, LANES), f32))
        peak[base : base + half, :] = top

    project(1, right_s)
    bounds = [pairs * c // chunks for c in range(chunks + 1)]

    def z_copy(source, c, direction):
        window = pl.ds(2 * bounds[c], 2 * (bounds[c + 1] - bounds[c]))
        toward = z + 1 - 2 * direction
        return pltpu.make_async_remote_copy(
            src_ref=right_all.at[source, window],
            dst_ref=right_all.at[source, window],
            send_sem=z_send.at[direction, source],
            recv_sem=z_recv.at[source, c],
            device_id={"gx": toward},
            device_id_type=MESH,
        )

    def left_copy(c):
        window = pl.ds(2 * bounds[c], 2 * (bounds[c + 1] - bounds[c]))
        return pltpu.make_async_remote_copy(
            src_ref=left_t.at[window],
            dst_ref=left_r.at[window],
            send_sem=l_send,
            recv_sem=l_recv.at[c],
            device_id={"gx": near},
            device_id_type=MESH,
        )

    pl.semaphore_wait(barrier, members)
    for c in range(chunks):
        for g in range(2 * bounds[c], 2 * bounds[c + 1]):
            tile = jnp.transpose(right_s[g * span : g * span + LANES, :])
            right_all[z, g] = tile[:cols].astype(bf16)

        @pl.when(z < nz - 1)
        def _():
            z_copy(z, c, 0).start()

        @pl.when(z > 0)
        def _():
            z_copy(z, c, 1).start()

    project(0, left_s)

    @pl.when(is_end)
    def _():
        for c in range(chunks):
            for g in range(2 * bounds[c], 2 * bounds[c + 1]):
                tile = jnp.transpose(left_s[g * span : g * span + LANES, :])
                left_t[g] = tile[:cols].astype(bf16)
            left_copy(c).start()

    for g in range(groups):
        left_b[g] = left_s[g * span : g * span + LANES, :].astype(bf16)

    peaks[me] = jnp.broadcast_to(jnp.max(jnp.transpose(peak[...]), axis=0, keepdims=True), (8, channels))

    def spread_peak(t, carry):
        peer = lax.rem(me + t, members)
        pltpu.make_async_remote_copy(
            src_ref=peaks.at[me],
            dst_ref=peaks.at[me],
            send_sem=peak_send,
            recv_sem=peak_recv,
            device_id={"gx": peer // ny, "gy": lax.rem(peer, ny)},
            device_id_type=MESH,
        ).start()
        return carry

    lax.fori_loop(1, members, spread_peak, 0)

    lane = lax.broadcasted_iota(jnp.int32, (rows, LANES), 1)

    def triangle_pair(lhs, r, p):
        halves = []
        for u in range(2):
            res = lax.dot_general(
                lhs[2 * p + u][:, :cols],
                right_all[r, 2 * p + u],
                (((1,), (0,)), ((), ())),
                preferred_element_type=f32,
            )
            t = res[:rows]
            for s in range(1, per):
                t = jnp.where(lane >= s * rows, res[s * rows : (s + 1) * rows], t)
            halves.append(t)
        return jnp.concatenate(halves, axis=0)

    def x_copy(rowset, target, sub, c, source):
        window = pl.ds(bounds[c], bounds[c + 1] - bounds[c])
        return pltpu.make_async_remote_copy(
            src_ref=send_t.at[rowset, target, sub, window],
            dst_ref=recv_t.at[rowset, source, sub, window],
            send_sem=x_send.at[rowset, target, sub],
            recv_sem=x_recv.at[rowset, source, sub, c],
            device_id={"gy": target},
            device_id_type=MESH,
        )

    def triangle_block(rowset, r, c):
        owner, sub = r // ratio, lax.rem(r, ratio)
        slot = jnp.where(owner == y, sub, ratio)
        lhs = left_e if rowset else left_b
        for p in range(bounds[c], bounds[c + 1]):
            t = triangle_pair(lhs, r, p)
            own_t[rowset, slot, p] = t
            send_t[rowset, owner, sub, p] = t.astype(bf16)

        @pl.when(owner != y)
        def _():
            x_copy(rowset, owner, sub, c, y).start()

    for c in range(chunks):
        triangle_block(0, z, c)

    def gate_step(b, carry):
        for u in range(unroll):
            i = b * unroll + u
            block = normed[pl.ds(pl.multiple_of(i * cols, 16), LANES), :]
            gating[i] = jax.nn.sigmoid(
                lax.dot_general(
                    gate_ref[...], block, (((1,), (1,)), ((), ())), preferred_element_type=f32
                )
            )
        return carry

    lax.fori_loop(0, rows // unroll, gate_step, 0)
    group_lane = lax.broadcasted_iota(jnp.int32, (1, LANES), 1)

    def lane_vector(scalar_of, g):
        ch = [jnp.minimum(g * per + s, half - 1) for s in range(per)]
        vector = jnp.full((1, LANES), scalar_of(ch[0]), f32)
        for s in range(1, per):
            vector = jnp.where(group_lane >= s * rows, scalar_of(ch[s]), vector)
        return vector

    def scale_of(ch):
        return (hist_smem[0, ch] / format_limit) * (hist_smem[1, ch] / format_limit)

    def fill_vectors(g, carry):
        vecs[0, pl.ds(g, 1), :] = lane_vector(scale_of, g)
        for cc in range(2):
            vecs[1 + cc, pl.ds(g, 1), :] = lane_vector(lambda ch: out_gain_smem[cc * half + ch], g)
            vecs[3 + cc, pl.ds(g, 1), :] = lane_vector(lambda ch: out_bias_smem[cc * half + ch], g)
        return carry

    lax.fori_loop(0, groups, fill_vectors, 0)

    def pair_vector(v, p):
        parts = [jnp.broadcast_to(vecs[v, 2 * p + u : 2 * p + u + 1, :], (rows, LANES)) for u in range(2)]
        return jnp.concatenate(parts, axis=0)

    def c_copy(sub, c):
        window = pl.ds(bounds[c], bounds[c + 1] - bounds[c])
        return pltpu.make_async_remote_copy(
            src_ref=full_t.at[col, sub, window],
            dst_ref=full_t.at[col, sub, window],
            send_sem=c_send.at[sub],
            recv_sem=c_recv.at[sub, c],
            device_id={"col": 1 - col},
            device_id_type=MESH,
        )

    def end_copy(sub, c):
        window = pl.ds(bounds[c], bounds[c + 1] - bounds[c])
        return pltpu.make_async_remote_copy(
            src_ref=ret_t.at[sub, window],
            dst_ref=full_t.at[col, sub, window],
            send_sem=e_send.at[sub],
            recv_sem=e_recv.at[sub, c],
            device_id={"gx": end},
            device_id_type=MESH,
        )

    def finish_block(rowset, r, c):
        owner, sub = r // ratio, lax.rem(r, ratio)

        @pl.when(owner == y)
        def _():
            def arrive(t, carry):
                x_copy(rowset, y, sub, c, lax.rem(y + t, ny)).wait_recv()
                return carry

            lax.fori_loop(1, ny, arrive, 0)
            for p in range(bounds[c], bounds[c + 1]):
                total = own_t[rowset, sub, p]
                for t in range(1, ny):
                    total = total + recv_t[rowset, lax.rem(y + t, ny), sub, p].astype(f32)
                result = (total * pair_vector(0, p)).astype(bf16)
                if rowset:
                    ret_t[sub, p] = result
                else:
                    full_t[col, sub, p] = result
            if rowset:
                end_copy(sub, c).start()
            else:
                c_copy(sub, c).start()

    row_at = lax.broadcasted_iota(jnp.int32, (2 * rows, LANES), 0) // rows
    lane_at = lax.broadcasted_iota(jnp.int32, (2 * rows, LANES), 1) // rows
    valid = (((pairs - 1) * 2 + row_at) * per + lane_at) < half

    def segment_mean(pair_sum):
        x = pair_sum[:rows] + pair_sum[rows:]
        total = x
        for s in range(1, per):
            total = total + pltpu.roll(x, s * rows, 1)
        result = total
        for s in range(1, per):
            moved = pltpu.roll(total, LANES - s * rows, 1)
            result = jnp.where(lane < (per - s) * rows, moved, result)
        result = result * (1.0 / channels)
        return jnp.concatenate([result, result], axis=0)

    def norm_sub(sub):
        for c in range(chunks):
            c_copy(sub, c).wait_recv()
        total = jnp.zeros((2 * rows, LANES), f32)
        for p in range(pairs):
            total = total + full_t[0, sub, p].astype(f32) + full_t[1, sub, p].astype(f32)
        mean = segment_mean(total)
        squares = jnp.zeros((2 * rows, LANES), f32)
        for p in range(pairs):
            for cc in range(2):
                square = jnp.square(full_t[cc, sub, p].astype(f32) - mean)
                if p == pairs - 1:
                    square = jnp.where(valid, square, 0.0)
                squares = squares + square
        factor = lax.rsqrt(segment_mean(squares) + epsilon)
        for p in range(pairs):
            for cc in range(2):
                t = (full_t[cc, sub, p].astype(f32) - mean) * factor
                t = t * pair_vector(1 + cc, p) + pair_vector(3 + cc, p)
                for ch in range(2 * p * per, min(2 * (p + 1) * per, half)):
                    u, s = ch // per - 2 * p, ch % per
                    piece = t[u * rows : (u + 1) * rows]
                    piece = pltpu.roll(piece, LANES - s * rows, 1) if s else piece
                    at = sub * (rows * pitch) + cc * half + ch
                    spread_t[pl.ds(at, rows, stride=pitch), :] = piece

    first_low = jnp.where(is_end, high_side, 2 * y < ny)
    order = jnp.where(first_low, ratio - 1, 0)
    step_sign = jnp.where(first_low, -1, 1)

    def norm_turn(turn):
        norm_sub(order + step_sign * turn)

    def return_block(r, c):
        owner, sub = r // ratio, lax.rem(r, ratio)

        @pl.when(owner == y)
        def _():
            end_copy(sub, c).wait_recv()
            c_copy(sub, c).start()

    within = nz == 4 and ratio == 2
    second = near - sgn

    @pl.when(is_next)
    def _():
        queue = [[(0, z, c) for c in range(chunks)]]
        for s in range(2 * chunks):
            k, c = 1 + s // chunks, s % chunks
            source = z - sgn * k
            if k == 1:
                z_copy(end, c, inward).wait_recv()
                z_copy(end, c, inward).start()
            elif within and c == chunks - 1:
                norm_turn(0)
            z_copy(source, c, 1 - inward).wait_recv()
            if k == 1:
                z_copy(source, c, 1 - inward).start()
                todo = [(0, source, c), (0, end, c)]
            else:
                left_copy(c).wait_recv()
                for g in range(2 * bounds[c], 2 * bounds[c + 1]):
                    tile = jnp.concatenate(
                        [left_r[g].astype(f32), jnp.zeros((LANES - cols, LANES), f32)], axis=0
                    )
                    left_e[g] = jnp.transpose(tile).astype(bf16)
                todo = [(1, source, c), (0, source, c)]
            for block in todo:
                triangle_block(*block)
            queue.append(todo)
            if s >= 2:
                for block in queue.pop(0):
                    finish_block(*block)
        for todo in queue:
            for block in todo:
                finish_block(*block)

        def farther(k, carry):
            for c in range(chunks):
                z_copy(z - sgn * k, c, 1 - inward).wait_recv()
                for rowset in (1, 0):
                    triangle_block(rowset, z - sgn * k, c)
                for rowset in (1, 0):
                    finish_block(rowset, z - sgn * k, c)
            return carry

        if nz > 4:
            lax.fori_loop(3, nz - 1, farther, 0)

    if nz > 4:

        @pl.when(jnp.logical_not(is_end | is_next))
        def _():
            def ring_step(d, carry):
                for c in range(chunks):
                    for source, direction, there in ((z - d, 0, z - d >= 0), (z + d, 1, z + d < nz)):

                        @pl.when(there)
                        def _(source=source, direction=direction, c=c):
                            z_copy(source, c, direction).wait_recv()
                            z_copy(source, c, direction).start()
                            triangle_block(0, source, c)
                            finish_block(0, source, c)

                return carry

            lax.fori_loop(1, nz - 1, ring_step, 0)
            for c in range(chunks):
                finish_block(0, z, c)

    @pl.when(is_end)
    def _():
        def arrived(source, c):
            z_copy(source, c, 1 - inward).wait_recv()
            triangle_block(0, source, c)

        def norm_if(here):
            if within:

                @pl.when(here)
                def _():
                    norm_turn(0)

        for c in range(chunks):
            arrived(near, c)
        for c in range(chunks):
            finish_block(0, z, c)
        arrived(second, 0)
        for c in range(chunks):
            finish_block(0, near, c)
        for c in range(1, chunks):
            if c == chunks // 2:
                norm_if(z // ratio == y)
            arrived(second, c)
            finish_block(0, second, c - 1)
        finish_block(0, second, chunks - 1)
        norm_if(z // ratio != y)

        def farther_back(k, carry):
            for c in range(chunks):
                return_block(near - sgn * k, c)
            return carry

        lax.fori_loop(2, nz - 1, farther_back, 0)

    for turn in range(1 if within else 0, ratio):
        norm_turn(turn)

    others = peaks.at[pl.ds(0, members - 1)]
    pltpu.make_async_copy(others, others, peak_recv).wait()
    top = jnp.max(jnp.max(peaks[...], axis=0), axis=0, keepdims=True)
    amax_ref[0:1, :] = top[:, :half]
    amax_ref[1:2, :] = top[:, half:]
    pltpu.make_async_copy(amax_ref, amax_hbm, amax_sem).start()

    wide = lax.broadcasted_iota(jnp.int32, (half, LANES), 1)

    def mix_step(b, carry):
        for u in range(unroll):
            i = b * unroll + u
            tiles = [
                spread_t[pl.ds((sub * rows + i) * pitch, channels), :].astype(bf16)
                for sub in range(ratio)
            ]
            res = jnp.dot(
                out_weight_ref[...], jnp.concatenate(tiles, axis=1), preferred_element_type=f32
            )
            mixing = res[:, :LANES]
            for sub in range(1, ratio):
                part = pltpu.roll(res[:, sub * LANES : (sub + 1) * LANES], sub * rows, 1)
                mixing = jnp.where(wide >= sub * rows, part, mixing)
            out_ref[i] = (gating[i] * mixing)[:, :cols].astype(bf16)
        window = pl.ds(b * unroll, unroll)
        pltpu.make_async_copy(out_ref.at[window], out_hbm.at[window], out_sem).start()
        return carry

    lax.fori_loop(0, rows // unroll, mix_step, 0)

    pltpu.make_async_copy(others, others, peak_send).wait()

    def sent(ref, sem):
        pltpu.make_async_copy(ref, ref, sem).wait()

    for sub in range(ratio):
        r = y * ratio + sub
        sent(full_t.at[col, sub], c_send.at[sub])

        @pl.when(is_next & (r != end) & (r != z) & (r != near))
        def _(sub=sub):
            sent(ret_t.at[sub], e_send.at[sub])

    def drain_x(t, carry):
        target = lax.rem(y + t, ny)
        for sub in range(ratio):
            r = target * ratio + sub

            @pl.when(jnp.logical_not(is_end) | (r == z) | (r == near) | (r == second))
            def _(sub=sub):
                sent(send_t.at[0, target, sub], x_send.at[0, target, sub])

            @pl.when(is_next & (r != end) & (r != z) & (r != near))
            def _(sub=sub):
                sent(send_t.at[1, target, sub], x_send.at[1, target, sub])

        return carry

    lax.fori_loop(1, ny, drain_x, 0)

    @pl.when(is_end)
    def _():
        sent(left_t, l_send)

    def drain_z(source, carry):
        @pl.when((source <= z) & (z < nz - 1) & ((source >= z - 1) | (z <= nz - 3)))
        def _():
            sent(right_all.at[source], z_send.at[0, source])

        @pl.when((source >= z) & (z > 0) & ((source <= z + 1) | (z >= 2)))
        def _():
            sent(right_all.at[source], z_send.at[1, source])

        return carry

    lax.fori_loop(0, nz, drain_z, 0)
    pltpu.make_async_copy(amax_ref, amax_hbm, amax_sem).wait()
    pltpu.make_async_copy(out_ref, out_hbm, out_sem).wait()


def on_device(
    nz,
    ny,
    pair_rep,
    pair_mask,
    amax_history,
    in_gain,
    in_bias,
    proj_weight,
    gate_weight,
    out_gain,
    out_bias,
    out_weight,
):
    crops, rows, cols, channels = pair_rep.shape
    half = proj_weight.shape[2]
    chunks = 4
    ratio = nz // ny
    per = LANES // rows
    pairs = -(-half // (2 * per))
    groups = 2 * pairs
    members = nz * ny
    weights = jnp.transpose(proj_weight, (1, 2, 0)).reshape(4 * half, channels)
    scratch_rows = -(-((groups - 1) * per * rows + LANES) // 8) * 8
    dma = pltpu.SemaphoreType.DMA
    vmem = pl.BlockSpec(memory_space=pltpu.VMEM)
    smem = pl.BlockSpec(memory_space=pltpu.SMEM)
    hbm = pl.BlockSpec(memory_space=pl.ANY)
    tile = (2 * rows, LANES)
    update, new_amax = pl.pallas_call(
        functools.partial(kernel, (nz, ny, rows, cols, half, chunks)),
        out_shape=(
            jax.ShapeDtypeStruct((rows, half, cols), bf16),
            jax.ShapeDtypeStruct((2, half), f32),
        ),
        in_specs=[vmem, vmem, vmem, smem, vmem, vmem, vmem, vmem, smem, smem, vmem],
        out_specs=(hbm, hbm),
        scratch_shapes=[
            pltpu.VMEM((rows * cols + LANES, channels), bf16),
            pltpu.VMEM((rows, LANES), f32),
            pltpu.VMEM((channels, LANES), f32),
            pltpu.VMEM((channels, LANES), f32),
            pltpu.VMEM((scratch_rows, LANES), f32),
            pltpu.VMEM((scratch_rows, LANES), f32),
            pltpu.VMEM((groups, LANES, LANES), bf16),
            pltpu.VMEM((groups, cols, LANES), bf16),
            pltpu.VMEM((groups, cols, LANES), bf16),
            pltpu.VMEM((groups, LANES, LANES), bf16),
            pltpu.VMEM((nz, groups, cols, LANES), bf16),
            pltpu.VMEM((2, ratio + 1, pairs) + tile, f32),
            pltpu.VMEM((2, ny, ratio, pairs) + tile, bf16),
            pltpu.VMEM((2, ny, ratio, pairs) + tile, bf16),
            pltpu.VMEM((ratio, pairs) + tile, bf16),
            pltpu.VMEM((2, ratio, pairs) + tile, bf16),
            pltpu.VMEM((ratio * rows * (channels + 1) + 8, LANES), f32),
            pltpu.VMEM((rows, half, cols), bf16),
            pltpu.VMEM((2, half), f32),
            pltpu.VMEM((5, groups, LANES), f32),
            pltpu.VMEM((rows, half, LANES), f32),
            pltpu.VMEM((members, 8, channels), f32),
            dma,
            dma,
            dma((2, nz)),
            dma((nz, chunks)),
            dma,
            dma((chunks,)),
            dma((2, ny, ratio)),
            dma((2, ny, ratio, chunks)),
            dma((ratio,)),
            dma((ratio, chunks)),
            dma((ratio,)),
            dma((ratio, chunks)),
            dma,
            dma,
        ],
        compiler_params=pltpu.CompilerParams(
            collective_id=0, has_side_effects=True, vmem_limit_bytes=56 * 1024 * 1024
        ),
    )(
        pair_rep[0],
        pair_mask[0],
        amax_history,
        amax_history,
        in_gain.reshape(1, channels),
        in_bias.reshape(1, channels),
        weights,
        gate_weight.T,
        out_gain,
        out_bias,
        out_weight.T,
    )
    return jnp.transpose(update, (0, 2, 1))[None], new_amax


def solution(mesh):
    placed = (
        P("ga", "gx", "gy", None),
        P("ga", "gx", "gy"),
        P(None, "col"),
        P(),
        P(),
        P(None, None, "col"),
        P(None, "col"),
        P(),
        P(),
        P(None, "col"),
    )
    return jax.shard_map(
        functools.partial(on_device, mesh.shape["gx"], mesh.shape["gy"]),
        mesh=mesh,
        in_specs=placed,
        out_specs=(P("ga", "gx", "gy", "col"), P("ga", "col")),
        check_vma=False,
    )
```

```python
import functools

import jax
import jax.numpy as jnp
from jax import lax
from jax.experimental import pallas as pl
from jax.experimental.pallas import tpu as pltpu
from jax.sharding import PartitionSpec as P

epsilon = 1e-05
format_limit = 448.0
LANES = 128
f32, bf16 = jnp.float32, jnp.bfloat16
MESH = pl.DeviceIdType.MESH


def kernel(
    dims,
    rep_ref,
    mask_ref,
    hist_ref,
    hist_smem,
    in_gain_ref,
    in_bias_ref,
    proj_ref,
    gate_ref,
    out_gain_smem,
    out_bias_smem,
    out_weight_ref,
    out_ref,
    amax_ref,
    normed,
    maskf,
    inverse,
    peak,
    left_s,
    right_s,
    left_b,
    left_t,
    left_r,
    left_e,
    right_all,
    own_t,
    send_t,
    recv_t,
    ret_t,
    full_t,
    spread_t,
    vecs,
    gating,
    peaks,
    peak_send,
    peak_recv,
    z_send,
    z_recv,
    l_send,
    l_recv,
    x_send,
    x_recv,
    c_send,
    c_recv,
    e_send,
    e_recv,
):
    nz, ny, rows, cols, half, chunks = dims
    ratio = nz // ny
    channels = 2 * half
    per = LANES // rows
    pairs = -(-half // (2 * per))
    groups = 2 * pairs
    span = per * rows
    pitch = channels + 1
    z, y, col = lax.axis_index("gx"), lax.axis_index("gy"), lax.axis_index("col")
    members = nz * ny
    me = z * ny + y
    is_end = (z == 0) | (z == nz - 1)
    is_next = (z == 1) | (z == nz - 2)
    high_side = 2 * z >= nz
    sgn = jnp.where(high_side, 1, -1)
    end = jnp.where(high_side, nz - 1, 0)
    inward = jnp.where(high_side, 1, 0)
    near = z - sgn
    unroll = max(u for u in range(1, 9) if rows % u == 0)

    barrier = pltpu.get_barrier_semaphore()

    def greet(t, carry):
        peer = lax.rem(me + t, members)
        pl.semaphore_signal(
            barrier, inc=1, device_id={"gx": peer // ny, "gy": lax.rem(peer, ny)}, device_id_type=MESH
        )
        return carry

    lax.fori_loop(1, members, greet, 0)
    pl.semaphore_signal(barrier, inc=1, device_id={"col": 1 - col}, device_id_type=MESH)

    normed[pl.ds(rows * cols, LANES), :] = jnp.zeros((LANES, channels), bf16)
    step_rows = unroll

    def norm_step(b, carry):
        values = rep_ref[pl.ds(b * step_rows, step_rows)].reshape(step_rows * cols, channels).astype(f32)
        average = jnp.mean(values, axis=-1, keepdims=True)
        centred = values - average
        var = jnp.mean(jnp.square(centred), axis=-1, keepdims=True)
        result = centred * lax.rsqrt(var + epsilon) * in_gain_ref[...] + in_bias_ref[...]
        start = pl.multiple_of(b * step_rows * cols, 16)
        normed[pl.ds(start, step_rows * cols), :] = result.astype(bf16)
        return carry

    lax.fori_loop(0, rows // step_rows, norm_step, 0)
    maskf[...] = jnp.zeros_like(maskf)
    maskf[:, 0:cols] = mask_ref[...].astype(f32)
    scaled = format_limit / hist_ref[...]
    flipped = jnp.concatenate([scaled[0:1], scaled[1:2]], axis=1)
    flipped = jnp.broadcast_to(flipped, (channels, channels))
    inverse[...] = jnp.transpose(flipped)
    peak[...] = jnp.zeros_like(peak)
    tail = left_s.shape[0] - half * rows
    left_s[pl.ds(half * rows, tail), :] = jnp.zeros((tail, LANES), f32)
    right_s[pl.ds(half * rows, tail), :] = jnp.zeros((tail, LANES), f32)

    def project(side, target):
        base = side * half

        def one(i):
            block = normed[pl.ds(pl.multiple_of(i * cols, 16), LANES), :]
            p = lax.dot_general(
                proj_ref[2 * base : 2 * base + channels, :],
                block,
                (((1,), (1,)), ((), ())),
                preferred_element_type=f32,
            )
            value = jax.nn.sigmoid(p[half:]) * p[:half] * maskf[pl.ds(i, 1), :]
            target[pl.ds(i, half, stride=rows), :] = jnp.clip(
                value * inverse[base : base + half, :], -format_limit, format_limit
            )
            return jnp.abs(value)

        def step(b, top):
            for u in range(unroll):
                top = jnp.maximum(top, one(b * unroll + u))
            return top

        top = lax.fori_loop(0, rows // unroll, step, jnp.zeros((half, LANES), f32))
        peak[base : base + half, :] = top

    project(1, right_s)
    bounds = [-(-pairs * c // chunks) for c in range(chunks + 1)]

    def z_copy(source, c, direction):
        window = pl.ds(2 * bounds[c], 2 * (bounds[c + 1] - bounds[c]))
        toward = z + 1 - 2 * direction
        return pltpu.make_async_remote_copy(
            src_ref=right_all.at[source, window],
            dst_ref=right_all.at[source, window],
            send_sem=z_send.at[direction, source],
            recv_sem=z_recv.at[source, c],
            device_id={"gx": toward},
            device_id_type=MESH,
        )

    def left_copy(c):
        window = pl.ds(2 * bounds[c], 2 * (bounds[c + 1] - bounds[c]))
        return pltpu.make_async_remote_copy(
            src_ref=left_t.at[window],
            dst_ref=left_r.at[window],
            send_sem=l_send,
            recv_sem=l_recv.at[c],
            device_id={"gx": near},
            device_id_type=MESH,
        )

    pl.semaphore_wait(barrier, members)
    for c in range(chunks):
        for g in range(2 * bounds[c], 2 * bounds[c + 1]):
            tile = jnp.transpose(right_s[g * span : g * span + LANES, :])
            right_all[z, g] = tile[:cols].astype(bf16)

        @pl.when(z < nz - 1)
        def _():
            z_copy(z, c, 0).start()

        @pl.when(z > 0)
        def _():
            z_copy(z, c, 1).start()

    project(0, left_s)

    @pl.when(is_end)
    def _():
        for c in range(chunks):
            for g in range(2 * bounds[c], 2 * bounds[c + 1]):
                tile = jnp.transpose(left_s[g * span : g * span + LANES, :])
                left_t[g] = tile[:cols].astype(bf16)
            left_copy(c).start()

    for g in range(groups):
        left_b[g] = left_s[g * span : g * span + LANES, :].astype(bf16)

    peaks[me] = jnp.broadcast_to(jnp.max(jnp.transpose(peak[...]), axis=0, keepdims=True), (8, channels))

    def spread_peak(t, carry):
        peer = lax.rem(me + t, members)
        pltpu.make_async_remote_copy(
            src_ref=peaks.at[me],
            dst_ref=peaks.at[me],
            send_sem=peak_send,
            recv_sem=peak_recv,
            device_id={"gx": peer // ny, "gy": lax.rem(peer, ny)},
            device_id_type=MESH,
        ).start()
        return carry

    lax.fori_loop(1, members, spread_peak, 0)

    lane = lax.broadcasted_iota(jnp.int32, (rows, LANES), 1)

    def triangle_pair(lhs, r, p):
        halves = []
        for u in range(2):
            res = lax.dot_general(
                lhs[2 * p + u][:, :cols],
                right_all[r, 2 * p + u],
                (((1,), (0,)), ((), ())),
                preferred_element_type=f32,
            )
            t = res[:rows]
            for s in range(1, per):
                t = jnp.where(lane >= s * rows, res[s * rows : (s + 1) * rows], t)
            halves.append(t)
        return jnp.concatenate(halves, axis=0)

    def x_copy(rowset, target, sub, c, source):
        window = pl.ds(bounds[c], bounds[c + 1] - bounds[c])
        return pltpu.make_async_remote_copy(
            src_ref=send_t.at[rowset, target, sub, window],
            dst_ref=recv_t.at[rowset, source, sub, window],
            send_sem=x_send.at[rowset, target, sub],
            recv_sem=x_recv.at[rowset, source, sub, c],
            device_id={"gy": target},
            device_id_type=MESH,
        )

    def triangle_block(rowset, r, c):
        owner, sub = r // ratio, lax.rem(r, ratio)
        slot = jnp.where(owner == y, sub, ratio)
        lhs = left_e if rowset else left_b
        for p in range(bounds[c], bounds[c + 1]):
            t = triangle_pair(lhs, r, p)
            own_t[rowset, slot, p] = t
            send_t[rowset, owner, sub, p] = t.astype(bf16)

        @pl.when(owner != y)
        def _():
            x_copy(rowset, owner, sub, c, y).start()

    for c in range(chunks):
        triangle_block(0, z, c)

    def gate_step(b, carry):
        for u in range(unroll):
            i = b * unroll + u
            block = normed[pl.ds(pl.multiple_of(i * cols, 16), LANES), :]
            gating[i] = jax.nn.sigmoid(
                lax.dot_general(
                    gate_ref[...], block, (((1,), (1,)), ((), ())), preferred_element_type=f32
                )
            )
        return carry

    lax.fori_loop(0, rows // unroll, gate_step, 0)
    group_lane = lax.broadcasted_iota(jnp.int32, (1, LANES), 1)

    def lane_vector(scalar_of, g):
        ch = [jnp.minimum(g * per + s, half - 1) for s in range(per)]
        vector = jnp.full((1, LANES), scalar_of(ch[0]), f32)
        for s in range(1, per):
            vector = jnp.where(group_lane >= s * rows, scalar_of(ch[s]), vector)
        return vector

    def scale_of(ch):
        return (hist_smem[0, ch] / format_limit) * (hist_smem[1, ch] / format_limit)

    def fill_vectors(g, carry):
        vecs[0, pl.ds(g, 1), :] = lane_vector(scale_of, g)
        for cc in range(2):
            vecs[1 + cc, pl.ds(g, 1), :] = lane_vector(lambda ch: out_gain_smem[cc * half + ch], g)
            vecs[3 + cc, pl.ds(g, 1), :] = lane_vector(lambda ch: out_bias_smem[cc * half + ch], g)
        return carry

    lax.fori_loop(0, groups, fill_vectors, 0)

    def pair_vector(v, p):
        parts = [jnp.broadcast_to(vecs[v, 2 * p + u : 2 * p + u + 1, :], (rows, LANES)) for u in range(2)]
        return jnp.concatenate(parts, axis=0)

    def c_copy(sub, c):
        window = pl.ds(bounds[c], bounds[c + 1] - bounds[c])
        return pltpu.make_async_remote_copy(
            src_ref=full_t.at[col, sub, window],
            dst_ref=full_t.at[col, sub, window],
            send_sem=c_send.at[sub],
            recv_sem=c_recv.at[sub, c],
            device_id={"col": 1 - col},
            device_id_type=MESH,
        )

    def end_copy(sub, c):
        window = pl.ds(bounds[c], bounds[c + 1] - bounds[c])
        return pltpu.make_async_remote_copy(
            src_ref=ret_t.at[sub, window],
            dst_ref=full_t.at[col, sub, window],
            send_sem=e_send.at[sub],
            recv_sem=e_recv.at[sub, c],
            device_id={"gx": end},
            device_id_type=MESH,
        )

    def finish_block(rowset, r, c):
        owner, sub = r // ratio, lax.rem(r, ratio)

        @pl.when(owner == y)
        def _():
            def arrive(t, carry):
                x_copy(rowset, y, sub, c, lax.rem(y + t, ny)).wait_recv()
                return carry

            lax.fori_loop(1, ny, arrive, 0)
            for p in range(bounds[c], bounds[c + 1]):
                total = own_t[rowset, sub, p]
                for t in range(1, ny):
                    total = total + recv_t[rowset, lax.rem(y + t, ny), sub, p].astype(f32)
                result = (total * pair_vector(0, p)).astype(bf16)
                if rowset:
                    ret_t[sub, p] = result
                else:
                    full_t[col, sub, p] = result
            if rowset:
                end_copy(sub, c).start()
            else:
                c_copy(sub, c).start()

    row_at = lax.broadcasted_iota(jnp.int32, (2 * rows, LANES), 0) // rows
    lane_at = lax.broadcasted_iota(jnp.int32, (2 * rows, LANES), 1) // rows
    valid = (((pairs - 1) * 2 + row_at) * per + lane_at) < half

    def segment_mean(pair_sum):
        x = pair_sum[:rows] + pair_sum[rows:]
        total = x
        for s in range(1, per):
            total = total + pltpu.roll(x, s * rows, 1)
        result = total
        for s in range(1, per):
            moved = pltpu.roll(total, LANES - s * rows, 1)
            result = jnp.where(lane < (per - s) * rows, moved, result)
        result = result * (1.0 / channels)
        return jnp.concatenate([result, result], axis=0)

    def norm_sub(sub):
        for c in range(chunks):
            c_copy(sub, c).wait_recv()
        total = jnp.zeros((2 * rows, LANES), f32)
        for p in range(pairs):
            total = total + full_t[0, sub, p].astype(f32) + full_t[1, sub, p].astype(f32)
        mean = segment_mean(total)
        squares = jnp.zeros((2 * rows, LANES), f32)
        for p in range(pairs):
            for cc in range(2):
                square = jnp.square(full_t[cc, sub, p].astype(f32) - mean)
                if p == pairs - 1:
                    square = jnp.where(valid, square, 0.0)
                squares = squares + square
        factor = lax.rsqrt(segment_mean(squares) + epsilon)
        for p in range(pairs):
            for cc in range(2):
                t = (full_t[cc, sub, p].astype(f32) - mean) * factor
                t = t * pair_vector(1 + cc, p) + pair_vector(3 + cc, p)
                for ch in range(2 * p * per, min(2 * (p + 1) * per, half)):
                    u, s = ch // per - 2 * p, ch % per
                    piece = t[u * rows : (u + 1) * rows]
                    piece = pltpu.roll(piece, LANES - s * rows, 1) if s else piece
                    at = sub * (rows * pitch) + cc * half + ch
                    spread_t[pl.ds(at, rows, stride=pitch), :] = piece

    first_low = jnp.where(is_end, high_side, 2 * y < ny)
    order = jnp.where(first_low, ratio - 1, 0)
    step_sign = jnp.where(first_low, -1, 1)

    def norm_turn(turn):
        norm_sub(order + step_sign * turn)

    def return_block(r, c):
        owner, sub = r // ratio, lax.rem(r, ratio)

        @pl.when(owner == y)
        def _():
            end_copy(sub, c).wait_recv()
            c_copy(sub, c).start()

    within = nz == 4 and ratio == 2
    second = near - sgn

    @pl.when(is_next)
    def _():
        queue = [[(0, z, c) for c in range(chunks)]]
        for s in range(2 * chunks):
            k, c = 1 + s // chunks, s % chunks
            source = z - sgn * k
            if k == 1:
                z_copy(end, c, inward).wait_recv()
                z_copy(end, c, inward).start()
            elif within and c == chunks - 1:
                norm_turn(0)
            z_copy(source, c, 1 - inward).wait_recv()
            if k == 1:
                z_copy(source, c, 1 - inward).start()
                todo = [(0, source, c), (0, end, c)]
            else:
                left_copy(c).wait_recv()
                for g in range(2 * bounds[c], 2 * bounds[c + 1]):
                    tile = jnp.concatenate(
                        [left_r[g].astype(f32), jnp.zeros((LANES - cols, LANES), f32)], axis=0
                    )
                    left_e[g] = jnp.transpose(tile).astype(bf16)
                todo = [(1, source, c), (0, source, c)]
            for block in todo:
                triangle_block(*block)
            queue.append(todo)
            if s >= 2:
                for block in queue.pop(0):
                    finish_block(*block)
            if s >= chunks and len(queue) > 2:
                for block in queue.pop(0):
                    finish_block(*block)
        for todo in queue:
            for block in todo:
                finish_block(*block)

        def farther(k, carry):
            for c in range(chunks):
                z_copy(z - sgn * k, c, 1 - inward).wait_recv()
                for rowset in (1, 0):
                    triangle_block(rowset, z - sgn * k, c)
                for rowset in (1, 0):
                    finish_block(rowset, z - sgn * k, c)
            return carry

        if nz > 4:
            lax.fori_loop(3, nz - 1, farther, 0)

    if nz > 4:

        @pl.when(jnp.logical_not(is_end | is_next))
        def _():
            def ring_step(d, carry):
                for c in range(chunks):
                    for source, direction, there in ((z - d, 0, z - d >= 0), (z + d, 1, z + d < nz)):

                        @pl.when(there)
                        def _(source=source, direction=direction, c=c):
                            z_copy(source, c, direction).wait_recv()
                            z_copy(source, c, direction).start()
                            triangle_block(0, source, c)
                            finish_block(0, source, c)

                return carry

            lax.fori_loop(1, nz - 1, ring_step, 0)
            for c in range(chunks):
                finish_block(0, z, c)

    @pl.when(is_end)
    def _():
        def arrived(source, c):
            z_copy(source, c, 1 - inward).wait_recv()
            triangle_block(0, source, c)

        def norm_if(here):
            if within:

                @pl.when(here)
                def _():
                    norm_turn(0)

        for c in range(chunks):
            arrived(near, c)
        for c in range(chunks):
            finish_block(0, z, c)
        arrived(second, 0)
        for c in range(chunks):
            finish_block(0, near, c)
        for c in range(1, chunks):
            if c == chunks // 2:
                norm_if(z // ratio == y)
            arrived(second, c)
            finish_block(0, second, c - 1)
        finish_block(0, second, chunks - 1)
        norm_if(z // ratio != y)

        def farther_back(k, carry):
            for c in range(chunks):
                return_block(near - sgn * k, c)
            return carry

        lax.fori_loop(2, nz - 1, farther_back, 0)

    for turn in range(1 if within else 0, ratio):
        norm_turn(turn)

    others = peaks.at[pl.ds(0, members - 1)]
    pltpu.make_async_copy(others, others, peak_recv).wait()
    top = jnp.max(jnp.max(peaks[...], axis=0), axis=0, keepdims=True)
    amax_ref[0:1, :] = top[:, :half]
    amax_ref[1:2, :] = top[:, half:]

    wide = lax.broadcasted_iota(jnp.int32, (half, LANES), 1)

    def mix_step(b, carry):
        for u in range(unroll):
            i = b * unroll + u
            tiles = [
                spread_t[pl.ds((sub * rows + i) * pitch, channels), :].astype(bf16)
                for sub in range(ratio)
            ]
            res = jnp.dot(
                out_weight_ref[...], jnp.concatenate(tiles, axis=1), preferred_element_type=f32
            )
            mixing = res[:, :LANES]
            for sub in range(1, ratio):
                part = pltpu.roll(res[:, sub * LANES : (sub + 1) * LANES], sub * rows, 1)
                mixing = jnp.where(wide >= sub * rows, part, mixing)
            out_ref[i] = (gating[i] * mixing)[:, :cols].astype(bf16)
        return carry

    lax.fori_loop(0, rows // unroll, mix_step, 0)

    pltpu.make_async_copy(others, others, peak_send).wait()

    def sent(ref, sem):
        pltpu.make_async_copy(ref, ref, sem).wait()

    for sub in range(ratio):
        r = y * ratio + sub
        sent(full_t.at[col, sub], c_send.at[sub])

        @pl.when(is_next & (r != end) & (r != z) & (r != near))
        def _(sub=sub):
            sent(ret_t.at[sub], e_send.at[sub])

    def drain_x(t, carry):
        target = lax.rem(y + t, ny)
        for sub in range(ratio):
            r = target * ratio + sub

            @pl.when(jnp.logical_not(is_end) | (r == z) | (r == near) | (r == second))
            def _(sub=sub):
                sent(send_t.at[0, target, sub], x_send.at[0, target, sub])

            @pl.when(is_next & (r != end) & (r != z) & (r != near))
            def _(sub=sub):
                sent(send_t.at[1, target, sub], x_send.at[1, target, sub])

        return carry

    lax.fori_loop(1, ny, drain_x, 0)

    @pl.when(is_end)
    def _():
        sent(left_t, l_send)

    def drain_z(source, carry):
        @pl.when((source <= z) & (z < nz - 1) & ((source >= z - 1) | (z <= nz - 3)))
        def _():
            sent(right_all.at[source], z_send.at[0, source])

        @pl.when((source >= z) & (z > 0) & ((source <= z + 1) | (z >= 2)))
        def _():
            sent(right_all.at[source], z_send.at[1, source])

        return carry

    lax.fori_loop(0, nz, drain_z, 0)


def on_device(
    nz,
    ny,
    pair_rep,
    pair_mask,
    amax_history,
    in_gain,
    in_bias,
    proj_weight,
    gate_weight,
    out_gain,
    out_bias,
    out_weight,
):
    crops, rows, cols, channels = pair_rep.shape
    half = proj_weight.shape[2]
    chunks = 5
    ratio = nz // ny
    per = LANES // rows
    pairs = -(-half // (2 * per))
    groups = 2 * pairs
    members = nz * ny
    weights = jnp.transpose(proj_weight, (1, 2, 0)).reshape(4 * half, channels)
    scratch_rows = -(-((groups - 1) * per * rows + LANES) // 8) * 8
    dma = pltpu.SemaphoreType.DMA
    vmem = pl.BlockSpec(memory_space=pltpu.VMEM)
    smem = pl.BlockSpec(memory_space=pltpu.SMEM)
    tile = (2 * rows, LANES)
    update, new_amax = pl.pallas_call(
        functools.partial(kernel, (nz, ny, rows, cols, half, chunks)),
        out_shape=(
            pltpu.VMEM((rows, half, cols), bf16),
            pltpu.VMEM((2, half), f32),
        ),
        in_specs=[vmem, vmem, vmem, smem, vmem, vmem, vmem, vmem, smem, smem, vmem],
        out_specs=(vmem, vmem),
        scratch_shapes=[
            pltpu.VMEM((rows * cols + LANES, channels), bf16),
            pltpu.VMEM((rows, LANES), f32),
            pltpu.VMEM((channels, LANES), f32),
            pltpu.VMEM((channels, LANES), f32),
            pltpu.VMEM((scratch_rows, LANES), f32),
            pltpu.VMEM((scratch_rows, LANES), f32),
            pltpu.VMEM((groups, LANES, LANES), bf16),
            pltpu.VMEM((groups, cols, LANES), bf16),
            pltpu.VMEM((groups, cols, LANES), bf16),
            pltpu.VMEM((groups, LANES, LANES), bf16),
            pltpu.VMEM((nz, groups, cols, LANES), bf16),
            pltpu.VMEM((2, ratio + 1, pairs) + tile, f32),
            pltpu.VMEM((2, ny, ratio, pairs) + tile, bf16),
            pltpu.VMEM((2, ny, ratio, pairs) + tile, bf16),
            pltpu.VMEM((ratio, pairs) + tile, bf16),
            pltpu.VMEM((2, ratio, pairs) + tile, bf16),
            pltpu.VMEM((ratio * rows * (channels + 1) + 8, LANES), f32),
            pltpu.VMEM((5, groups, LANES), f32),
            pltpu.VMEM((rows, half, LANES), f32),
            pltpu.VMEM((members, 8, channels), f32),
            dma,
            dma,
            dma((2, nz)),
            dma((nz, chunks)),
            dma,
            dma((chunks,)),
            dma((2, ny, ratio)),
            dma((2, ny, ratio, chunks)),
            dma((ratio,)),
            dma((ratio, chunks)),
            dma((ratio,)),
            dma((ratio, chunks)),
        ],
        compiler_params=pltpu.CompilerParams(
            collective_id=0, has_side_effects=True, vmem_limit_bytes=56 * 1024 * 1024
        ),
    )(
        pair_rep[0],
        pair_mask[0],
        amax_history,
        amax_history,
        in_gain.reshape(1, channels),
        in_bias.reshape(1, channels),
        weights,
        gate_weight.T,
        out_gain,
        out_bias,
        out_weight.T,
    )
    return jnp.transpose(update, (0, 2, 1))[None], new_amax


def solution(mesh):
    placed = (
        P("ga", "gx", "gy", None),
        P("ga", "gx", "gy"),
        P(None, "col"),
        P(),
        P(),
        P(None, None, "col"),
        P(None, "col"),
        P(),
        P(),
        P(None, "col"),
    )
    return jax.shard_map(
        functools.partial(on_device, mesh.shape["gx"], mesh.shape["gy"]),
        mesh=mesh,
        in_specs=placed,
        out_specs=(P("ga", "gx", "gy", "col"), P("ga", "col")),
        check_vma=False,
    )
```

```python
import functools

import jax
import jax.numpy as jnp
from jax import lax
from jax.experimental import pallas as pl
from jax.experimental.pallas import tpu as pltpu
from jax.sharding import PartitionSpec as P

epsilon = 1e-05
format_limit = 448.0
LANES = 128
f32, bf16 = jnp.float32, jnp.bfloat16
MESH = pl.DeviceIdType.MESH


def kernel(
    dims,
    rep_ref,
    mask_ref,
    hist_ref,
    hist_smem,
    in_gain_ref,
    in_bias_ref,
    proj_ref,
    gate_ref,
    out_gain_smem,
    out_bias_smem,
    out_weight_ref,
    out_ref,
    amax_ref,
    normed,
    maskf,
    inverse,
    peak,
    left_s,
    right_s,
    left_b,
    left_t,
    left_r,
    left_e,
    right_all,
    own_t,
    send_t,
    recv_t,
    ret_t,
    full_t,
    spread_t,
    vecs,
    mixed,
    gating,
    peaks,
    peak_send,
    peak_recv,
    z_send,
    z_recv,
    l_send,
    l_recv,
    x_send,
    x_recv,
    c_send,
    c_recv,
    e_send,
    e_recv,
):
    nz, ny, rows, cols, half, chunks = dims
    ratio = nz // ny
    channels = 2 * half
    per = LANES // rows
    pairs = -(-half // (2 * per))
    groups = 2 * pairs
    span = per * rows
    pitch = channels + 1
    z, y, col = lax.axis_index("gx"), lax.axis_index("gy"), lax.axis_index("col")
    members = nz * ny
    me = z * ny + y
    is_end = (z == 0) | (z == nz - 1)
    is_next = (z == 1) | (z == nz - 2)
    high_side = 2 * z >= nz
    sgn = jnp.where(high_side, 1, -1)
    end = jnp.where(high_side, nz - 1, 0)
    inward = jnp.where(high_side, 1, 0)
    near = z - sgn

    def steps(limit):
        return max(u for u in range(1, limit + 1) if rows % u == 0)

    step_rows, project_rows, gate_rows, mix_rows = steps(40), steps(40), steps(40), steps(40)

    barrier = pltpu.get_barrier_semaphore()

    def greet(t, carry):
        peer = lax.rem(me + t, members)
        pl.semaphore_signal(
            barrier, inc=1, device_id={"gx": peer // ny, "gy": lax.rem(peer, ny)}, device_id_type=MESH
        )
        return carry

    lax.fori_loop(1, members, greet, 0)
    pl.semaphore_signal(barrier, inc=1, device_id={"col": 1 - col}, device_id_type=MESH)

    normed[pl.ds(rows * cols, LANES), :] = jnp.zeros((LANES, channels), bf16)

    ones = jnp.ones((channels, channels), bf16)

    def norm_step(b, carry):
        values = rep_ref[pl.ds(b * step_rows, step_rows)].reshape(step_rows * cols, channels)
        average = jnp.dot(values, ones, preferred_element_type=f32) * (1.0 / channels)
        centred = values.astype(f32) - average
        var = jnp.mean(jnp.square(centred), axis=-1, keepdims=True)
        result = centred * lax.rsqrt(var + epsilon) * in_gain_ref[...] + in_bias_ref[...]
        start = pl.multiple_of(b * step_rows * cols, 16)
        normed[pl.ds(start, step_rows * cols), :] = result.astype(bf16)
        return carry

    lax.fori_loop(0, rows // step_rows, norm_step, 0)
    maskf[...] = jnp.zeros_like(maskf)
    maskf[:, 0:cols] = mask_ref[...].astype(f32)
    scaled = format_limit / hist_ref[...]
    flipped = jnp.concatenate([scaled[0:1], scaled[1:2]], axis=1)
    flipped = jnp.broadcast_to(flipped, (channels, channels))
    inverse[...] = jnp.transpose(flipped)
    peak[...] = jnp.zeros_like(peak)
    tail = left_s.shape[0] - half * rows
    left_s[pl.ds(half * rows, tail), :] = jnp.zeros((tail, LANES), f32)
    right_s[pl.ds(half * rows, tail), :] = jnp.zeros((tail, LANES), f32)

    def project(side, target):
        base = side * half

        def one(i):
            block = normed[pl.ds(pl.multiple_of(i * cols, 16), LANES), :]
            p = lax.dot_general(
                proj_ref[2 * base : 2 * base + channels, :],
                block,
                (((1,), (1,)), ((), ())),
                preferred_element_type=f32,
            )
            value = jax.nn.sigmoid(p[half:]) * p[:half] * maskf[pl.ds(i, 1), :]
            target[pl.ds(i, half, stride=rows), :] = jnp.clip(
                value * inverse[base : base + half, :], -format_limit, format_limit
            )
            return jnp.abs(value)

        def step(b, top):
            for u in range(project_rows):
                top = jnp.maximum(top, one(b * project_rows + u))
            return top

        top = lax.fori_loop(0, rows // project_rows, step, jnp.zeros((half, LANES), f32))
        peak[base : base + half, :] = top

    project(1, right_s)
    bounds = [-(-pairs * c // chunks) for c in range(chunks + 1)]

    def z_copy(source, c, direction):
        window = pl.ds(2 * bounds[c], 2 * (bounds[c + 1] - bounds[c]))
        toward = z + 1 - 2 * direction
        return pltpu.make_async_remote_copy(
            src_ref=right_all.at[source, window],
            dst_ref=right_all.at[source, window],
            send_sem=z_send.at[direction, source],
            recv_sem=z_recv.at[source, c],
            device_id={"gx": toward},
            device_id_type=MESH,
        )

    def left_copy(c):
        window = pl.ds(2 * bounds[c], 2 * (bounds[c + 1] - bounds[c]))
        return pltpu.make_async_remote_copy(
            src_ref=left_t.at[window],
            dst_ref=left_r.at[window],
            send_sem=l_send,
            recv_sem=l_recv.at[c],
            device_id={"gx": near},
            device_id_type=MESH,
        )

    pl.semaphore_wait(barrier, members)
    for c in range(chunks):
        for g in range(2 * bounds[c], 2 * bounds[c + 1]):
            tile = jnp.transpose(right_s[g * span : g * span + LANES, :])
            right_all[z, g] = tile[:cols].astype(bf16)

        @pl.when(z < nz - 1)
        def _():
            z_copy(z, c, 0).start()

        @pl.when(z > 0)
        def _():
            z_copy(z, c, 1).start()

    project(0, left_s)

    @pl.when(is_end)
    def _():
        for c in range(chunks):
            for g in range(2 * bounds[c], 2 * bounds[c + 1]):
                tile = jnp.transpose(left_s[g * span : g * span + LANES, :])
                left_t[g] = tile[:cols].astype(bf16)
            left_copy(c).start()

    for g in range(groups):
        left_b[g] = left_s[g * span : g * span + LANES, :].astype(bf16)

    peaks[me] = jnp.broadcast_to(jnp.max(jnp.transpose(peak[...]), axis=0, keepdims=True), (8, channels))

    def spread_peak(t, carry):
        peer = lax.rem(me + t, members)
        pltpu.make_async_remote_copy(
            src_ref=peaks.at[me],
            dst_ref=peaks.at[me],
            send_sem=peak_send,
            recv_sem=peak_recv,
            device_id={"gx": peer // ny, "gy": lax.rem(peer, ny)},
            device_id_type=MESH,
        ).start()
        return carry

    lax.fori_loop(1, members, spread_peak, 0)

    lane = lax.broadcasted_iota(jnp.int32, (rows, LANES), 1)

    def triangle_pair(lhs, r, p):
        halves = []
        for u in range(2):
            res = lax.dot_general(
                lhs[2 * p + u][:, :cols],
                right_all[r, 2 * p + u],
                (((1,), (0,)), ((), ())),
                preferred_element_type=f32,
            )
            t = res[:rows]
            for s in range(1, per):
                t = jnp.where(lane >= s * rows, res[s * rows : (s + 1) * rows], t)
            halves.append(t)
        return jnp.concatenate(halves, axis=0)

    def x_copy(rowset, target, sub, c, source):
        window = pl.ds(bounds[c], bounds[c + 1] - bounds[c])
        return pltpu.make_async_remote_copy(
            src_ref=send_t.at[rowset, target, sub, window],
            dst_ref=recv_t.at[rowset, source, sub, window],
            send_sem=x_send.at[rowset, target, sub],
            recv_sem=x_recv.at[rowset, source, sub, c],
            device_id={"gy": target},
            device_id_type=MESH,
        )

    def triangle_block(rowset, r, c):
        owner, sub = r // ratio, lax.rem(r, ratio)
        slot = jnp.where(owner == y, sub, ratio)
        lhs = left_e if rowset else left_b
        for p in range(bounds[c], bounds[c + 1]):
            t = triangle_pair(lhs, r, p)
            own_t[rowset, slot, p] = t
            send_t[rowset, owner, sub, p] = t.astype(bf16)

        @pl.when(owner != y)
        def _():
            x_copy(rowset, owner, sub, c, y).start()

    for c in range(chunks):
        triangle_block(0, z, c)

    def gate_step(b, carry):
        for u in range(gate_rows):
            i = b * gate_rows + u
            block = normed[pl.ds(pl.multiple_of(i * cols, 16), LANES), :]
            gating[i] = jax.nn.sigmoid(
                lax.dot_general(
                    gate_ref[...], block, (((1,), (1,)), ((), ())), preferred_element_type=f32
                )
            )
        return carry

    lax.fori_loop(0, rows // gate_rows, gate_step, 0)
    group_lane = lax.broadcasted_iota(jnp.int32, (1, LANES), 1)

    def lane_vector(scalar_of, g):
        ch = [jnp.minimum(g * per + s, half - 1) for s in range(per)]
        vector = jnp.full((1, LANES), scalar_of(ch[0]), f32)
        for s in range(1, per):
            vector = jnp.where(group_lane >= s * rows, scalar_of(ch[s]), vector)
        return vector

    def scale_of(ch):
        return (hist_smem[0, ch] / format_limit) * (hist_smem[1, ch] / format_limit)

    def fill_vectors(g, carry):
        vecs[0, pl.ds(g, 1), :] = lane_vector(scale_of, g)
        for cc in range(2):
            vecs[1 + cc, pl.ds(g, 1), :] = lane_vector(lambda ch: out_gain_smem[cc * half + ch], g)
            vecs[3 + cc, pl.ds(g, 1), :] = lane_vector(lambda ch: out_bias_smem[cc * half + ch], g)
        return carry

    lax.fori_loop(0, groups, fill_vectors, 0)

    def pair_vector(v, p):
        parts = [jnp.broadcast_to(vecs[v, 2 * p + u : 2 * p + u + 1, :], (rows, LANES)) for u in range(2)]
        return jnp.concatenate(parts, axis=0)

    def c_copy(sub, c):
        window = pl.ds(bounds[c], bounds[c + 1] - bounds[c])
        return pltpu.make_async_remote_copy(
            src_ref=full_t.at[col, sub, window],
            dst_ref=full_t.at[col, sub, window],
            send_sem=c_send.at[sub],
            recv_sem=c_recv.at[sub, c],
            device_id={"col": 1 - col},
            device_id_type=MESH,
        )

    def end_copy(sub, c):
        window = pl.ds(bounds[c], bounds[c + 1] - bounds[c])
        return pltpu.make_async_remote_copy(
            src_ref=ret_t.at[sub, window],
            dst_ref=full_t.at[col, sub, window],
            send_sem=e_send.at[sub],
            recv_sem=e_recv.at[sub, c],
            device_id={"gx": end},
            device_id_type=MESH,
        )

    def finish_block(rowset, r, c):
        owner, sub = r // ratio, lax.rem(r, ratio)

        @pl.when(owner == y)
        def _():
            def arrive(t, carry):
                x_copy(rowset, y, sub, c, lax.rem(y + t, ny)).wait_recv()
                return carry

            lax.fori_loop(1, ny, arrive, 0)
            for p in range(bounds[c], bounds[c + 1]):
                total = own_t[rowset, sub, p]
                for t in range(1, ny):
                    total = total + recv_t[rowset, lax.rem(y + t, ny), sub, p].astype(f32)
                result = (total * pair_vector(0, p)).astype(bf16)
                if rowset:
                    ret_t[sub, p] = result
                else:
                    full_t[col, sub, p] = result
            if rowset:
                end_copy(sub, c).start()
            else:
                c_copy(sub, c).start()

    row_at = lax.broadcasted_iota(jnp.int32, (2 * rows, LANES), 0) // rows
    lane_at = lax.broadcasted_iota(jnp.int32, (2 * rows, LANES), 1) // rows
    valid = (((pairs - 1) * 2 + row_at) * per + lane_at) < half

    def segment_mean(pair_sum):
        x = pair_sum[:rows] + pair_sum[rows:]
        total = x
        for s in range(1, per):
            total = total + pltpu.roll(x, s * rows, 1)
        result = total
        for s in range(1, per):
            moved = pltpu.roll(total, LANES - s * rows, 1)
            result = jnp.where(lane < (per - s) * rows, moved, result)
        result = result * (1.0 / channels)
        return jnp.concatenate([result, result], axis=0)

    def norm_sub(sub):
        for c in range(chunks):
            c_copy(sub, c).wait_recv()
        total = jnp.zeros((2 * rows, LANES), f32)
        for p in range(pairs):
            total = total + full_t[0, sub, p].astype(f32) + full_t[1, sub, p].astype(f32)
        mean = segment_mean(total)
        squares = jnp.zeros((2 * rows, LANES), f32)
        for p in range(pairs):
            for cc in range(2):
                square = jnp.square(full_t[cc, sub, p].astype(f32) - mean)
                if p == pairs - 1:
                    square = jnp.where(valid, square, 0.0)
                squares = squares + square
        factor = lax.rsqrt(segment_mean(squares) + epsilon)
        for p in range(pairs):
            for cc in range(2):
                t = (full_t[cc, sub, p].astype(f32) - mean) * factor
                t = t * pair_vector(1 + cc, p) + pair_vector(3 + cc, p)
                for ch in range(2 * p * per, min(2 * (p + 1) * per, half)):
                    u, s = ch // per - 2 * p, ch % per
                    piece = t[u * rows : (u + 1) * rows]
                    piece = pltpu.roll(piece, LANES - s * rows, 1) if s else piece
                    at = sub * (rows * pitch) + cc * half + ch
                    spread_t[pl.ds(at, rows, stride=pitch), :] = piece

    first_low = jnp.where(is_end, high_side, 2 * y < ny)
    order = jnp.where(first_low, ratio - 1, 0)
    step_sign = jnp.where(first_low, -1, 1)

    def norm_turn(turn):
        norm_sub(order + step_sign * turn)

    wide = lax.broadcasted_iota(jnp.int32, (half, LANES), 1)

    def mix_turn(turn):
        sub = order + step_sign * turn
        inside = (wide >= sub * rows) & (wide < (sub + 1) * rows)

        def mix_step(b, carry):
            for u in range(mix_rows):
                i = b * mix_rows + u
                tile = spread_t[pl.ds((sub * rows + i) * pitch, channels), :].astype(bf16)
                mixing = jnp.dot(out_weight_ref[...], tile, preferred_element_type=f32)
                mixing = pltpu.roll(mixing, sub * rows, 1)
                if turn:
                    mixing = jnp.where(inside, mixing, mixed[i])
                if turn < ratio - 1:
                    mixed[i] = mixing
                else:
                    out_ref[i] = (gating[i] * mixing)[:, :cols].astype(bf16)
            return carry

        lax.fori_loop(0, rows // mix_rows, mix_step, 0)

    def return_block(r, c):
        owner, sub = r // ratio, lax.rem(r, ratio)

        @pl.when(owner == y)
        def _():
            end_copy(sub, c).wait_recv()
            c_copy(sub, c).start()

    within = nz == 4 and ratio == 2
    second = near - sgn

    @pl.when(is_next)
    def _():
        queue = [[(0, z, c) for c in range(chunks)]]
        for s in range(2 * chunks):
            k, c = 1 + s // chunks, s % chunks
            source = z - sgn * k
            if k == 1:
                z_copy(end, c, inward).wait_recv()
                z_copy(end, c, inward).start()
            z_copy(source, c, 1 - inward).wait_recv()
            if k == 1:
                z_copy(source, c, 1 - inward).start()
                todo = [(0, source, c), (0, end, c)]
            else:
                left_copy(c).wait_recv()
                for g in range(2 * bounds[c], 2 * bounds[c + 1]):
                    tile = jnp.concatenate(
                        [left_r[g].astype(f32), jnp.zeros((LANES - cols, LANES), f32)], axis=0
                    )
                    left_e[g] = jnp.transpose(tile).astype(bf16)
                todo = [(1, source, c), (0, source, c)]
            for block in todo:
                triangle_block(*block)
            queue.append(todo)
            if s >= 2:
                for block in queue.pop(0):
                    finish_block(*block)
            if s >= chunks and len(queue) > 2:
                for block in queue.pop(0):
                    finish_block(*block)
        if within:
            norm_turn(0)
        for todo in queue:
            for block in todo:
                finish_block(*block)
        if within:
            mix_turn(0)

        def farther(k, carry):
            for c in range(chunks):
                z_copy(z - sgn * k, c, 1 - inward).wait_recv()
                for rowset in (1, 0):
                    triangle_block(rowset, z - sgn * k, c)
                for rowset in (1, 0):
                    finish_block(rowset, z - sgn * k, c)
            return carry

        if nz > 4:
            lax.fori_loop(3, nz - 1, farther, 0)

    if nz > 4:

        @pl.when(jnp.logical_not(is_end | is_next))
        def _():
            def ring_step(d, carry):
                for c in range(chunks):
                    for source, direction, there in ((z - d, 0, z - d >= 0), (z + d, 1, z + d < nz)):

                        @pl.when(there)
                        def _(source=source, direction=direction, c=c):
                            z_copy(source, c, direction).wait_recv()
                            z_copy(source, c, direction).start()
                            triangle_block(0, source, c)
                            finish_block(0, source, c)

                return carry

            lax.fori_loop(1, nz - 1, ring_step, 0)
            for c in range(chunks):
                finish_block(0, z, c)

    @pl.when(is_end)
    def _():
        def arrived(source, c):
            z_copy(source, c, 1 - inward).wait_recv()
            triangle_block(0, source, c)

        def norm_if(here):
            if within:

                @pl.when(here)
                def _():
                    norm_turn(0)

        for c in range(chunks):
            arrived(near, c)
        for c in range(chunks):
            finish_block(0, z, c)
        arrived(second, 0)
        for c in range(chunks):
            finish_block(0, near, c)
        for c in range(1, chunks):
            if c == chunks // 2:
                norm_if(z // ratio == y)
            arrived(second, c)
            finish_block(0, second, c - 1)
        finish_block(0, second, chunks - 1)
        norm_if(z // ratio != y)
        if within:
            mix_turn(0)

        def farther_back(k, carry):
            for c in range(chunks):
                return_block(near - sgn * k, c)
            return carry

        lax.fori_loop(2, nz - 1, farther_back, 0)

    others = peaks.at[pl.ds(0, members - 1)]
    pltpu.make_async_copy(others, others, peak_recv).wait()
    top = jnp.max(jnp.max(peaks[...], axis=0), axis=0, keepdims=True)
    amax_ref[0:1, :] = top[:, :half]
    amax_ref[1:2, :] = top[:, half:]

    pltpu.make_async_copy(others, others, peak_send).wait()

    def sent(ref, sem):
        pltpu.make_async_copy(ref, ref, sem).wait()

    def drain_x(t, carry):
        target = lax.rem(y + t, ny)
        for sub in range(ratio):
            r = target * ratio + sub

            @pl.when(jnp.logical_not(is_end) | (r == z) | (r == near) | (r == second))
            def _(sub=sub):
                sent(send_t.at[0, target, sub], x_send.at[0, target, sub])

            @pl.when(is_next & (r != end) & (r != z) & (r != near))
            def _(sub=sub):
                sent(send_t.at[1, target, sub], x_send.at[1, target, sub])

        return carry

    lax.fori_loop(1, ny, drain_x, 0)

    @pl.when(is_end)
    def _():
        sent(left_t, l_send)

    def drain_z(source, carry):
        @pl.when((source <= z) & (z < nz - 1) & ((source >= z - 1) | (z <= nz - 3)))
        def _():
            sent(right_all.at[source], z_send.at[0, source])

        @pl.when((source >= z) & (z > 0) & ((source <= z + 1) | (z >= 2)))
        def _():
            sent(right_all.at[source], z_send.at[1, source])

        return carry

    lax.fori_loop(0, nz, drain_z, 0)

    for turn in range(1 if within else 0, ratio):
        norm_turn(turn)
        mix_turn(turn)

    for sub in range(ratio):
        r = y * ratio + sub
        sent(full_t.at[col, sub], c_send.at[sub])

        @pl.when(is_next & (r != end) & (r != z) & (r != near))
        def _(sub=sub):
            sent(ret_t.at[sub], e_send.at[sub])


def on_device(
    nz,
    ny,
    pair_rep,
    pair_mask,
    amax_history,
    in_gain,
    in_bias,
    proj_weight,
    gate_weight,
    out_gain,
    out_bias,
    out_weight,
):
    crops, rows, cols, channels = pair_rep.shape
    half = proj_weight.shape[2]
    chunks = 5
    ratio = nz // ny
    per = LANES // rows
    pairs = -(-half // (2 * per))
    groups = 2 * pairs
    members = nz * ny
    weights = jnp.transpose(proj_weight, (1, 2, 0)).reshape(4 * half, channels)
    scratch_rows = -(-((groups - 1) * per * rows + LANES) // 8) * 8
    dma = pltpu.SemaphoreType.DMA
    vmem = pl.BlockSpec(memory_space=pltpu.VMEM)
    smem = pl.BlockSpec(memory_space=pltpu.SMEM)
    tile = (2 * rows, LANES)
    update, new_amax = pl.pallas_call(
        functools.partial(kernel, (nz, ny, rows, cols, half, chunks)),
        out_shape=(
            pltpu.VMEM((rows, half, cols), bf16),
            pltpu.VMEM((2, half), f32),
        ),
        in_specs=[vmem, vmem, vmem, smem, vmem, vmem, vmem, vmem, smem, smem, vmem],
        out_specs=(vmem, vmem),
        scratch_shapes=[
            pltpu.VMEM((rows * cols + LANES, channels), bf16),
            pltpu.VMEM((rows, LANES), f32),
            pltpu.VMEM((channels, LANES), f32),
            pltpu.VMEM((channels, LANES), f32),
            pltpu.VMEM((scratch_rows, LANES), f32),
            pltpu.VMEM((scratch_rows, LANES), f32),
            pltpu.VMEM((groups, LANES, LANES), bf16),
            pltpu.VMEM((groups, cols, LANES), bf16),
            pltpu.VMEM((groups, cols, LANES), bf16),
            pltpu.VMEM((groups, LANES, LANES), bf16),
            pltpu.VMEM((nz, groups, cols, LANES), bf16),
            pltpu.VMEM((2, ratio + 1, pairs) + tile, f32),
            pltpu.VMEM((2, ny, ratio, pairs) + tile, bf16),
            pltpu.VMEM((2, ny, ratio, pairs) + tile, bf16),
            pltpu.VMEM((ratio, pairs) + tile, bf16),
            pltpu.VMEM((2, ratio, pairs) + tile, bf16),
            pltpu.VMEM((ratio * rows * (channels + 1) + 8, LANES), f32),
            pltpu.VMEM((5, groups, LANES), f32),
            pltpu.VMEM((rows, half, LANES), f32),
            pltpu.VMEM((rows, half, LANES), f32),
            pltpu.VMEM((members, 8, channels), f32),
            dma,
            dma,
            dma((2, nz)),
            dma((nz, chunks)),
            dma,
            dma((chunks,)),
            dma((2, ny, ratio)),
            dma((2, ny, ratio, chunks)),
            dma((ratio,)),
            dma((ratio, chunks)),
            dma((ratio,)),
            dma((ratio, chunks)),
        ],
        compiler_params=pltpu.CompilerParams(
            collective_id=0, has_side_effects=True, vmem_limit_bytes=56 * 1024 * 1024
        ),
    )(
        pair_rep[0],
        pair_mask[0],
        amax_history,
        amax_history,
        in_gain.reshape(1, channels),
        in_bias.reshape(1, channels),
        weights,
        gate_weight.T,
        out_gain,
        out_bias,
        out_weight.T,
    )
    return jnp.transpose(update, (0, 2, 1))[None], new_amax


def solution(mesh):
    placed = (
        P("ga", "gx", "gy", None),
        P("ga", "gx", "gy"),
        P(None, "col"),
        P(),
        P(),
        P(None, None, "col"),
        P(None, "col"),
        P(),
        P(),
        P(None, "col"),
    )
    return jax.shard_map(
        functools.partial(on_device, mesh.shape["gx"], mesh.shape["gy"]),
        mesh=mesh,
        in_specs=placed,
        out_specs=(P("ga", "gx", "gy", "col"), P("ga", "col")),
        check_vma=False,
    )
```

```python
import functools

import jax
import jax.numpy as jnp
from jax import lax
from jax.experimental import pallas as pl
from jax.experimental.pallas import tpu as pltpu
from jax.sharding import PartitionSpec as P

epsilon = 1e-05
format_limit = 448.0
LANES = 128
f32, bf16 = jnp.float32, jnp.bfloat16
MESH = pl.DeviceIdType.MESH


def kernel(
    dims,
    rep_ref,
    mask_ref,
    hist_ref,
    hist_smem,
    in_gain_ref,
    in_bias_ref,
    proj_ref,
    gate_ref,
    out_gain_smem,
    out_bias_smem,
    out_weight_ref,
    out_ref,
    amax_ref,
    normed,
    maskf,
    inverse,
    peak,
    left_s,
    right_s,
    left_b,
    left_t,
    left_r,
    left_e,
    right_all,
    own_t,
    send_t,
    recv_t,
    full_t,
    spread_t,
    vecs,
    mixed,
    gating,
    peaks,
    peak_send,
    peak_recv,
    z_send,
    z_recv,
    l_send,
    l_recv,
    x_send,
    x_recv,
    c_send,
    c_recv,
):
    nz, ny, rows, cols, half, chunks = dims
    ratio = nz // ny
    channels = 2 * half
    per = LANES // rows
    pairs = -(-half // (2 * per))
    groups = 2 * pairs
    span = per * rows
    pitch = channels + 1
    z, y, col = lax.axis_index("gx"), lax.axis_index("gy"), lax.axis_index("col")
    members = nz * ny
    me = z * ny + y
    is_end = (z == 0) | (z == nz - 1)
    is_next = (z == 1) | (z == nz - 2)
    high_side = 2 * z >= nz
    sgn = jnp.where(high_side, 1, -1)
    end = jnp.where(high_side, nz - 1, 0)
    inward = jnp.where(high_side, 1, 0)
    near = z - sgn

    def steps(limit):
        return max(u for u in range(1, limit + 1) if rows % u == 0)

    step_rows, project_rows, gate_rows, mix_rows = steps(40), steps(40), steps(40), steps(40)

    barrier = pltpu.get_barrier_semaphore()

    def greet(t, carry):
        peer = lax.rem(me + t, members)
        pl.semaphore_signal(
            barrier, inc=1, device_id={"gx": peer // ny, "gy": lax.rem(peer, ny)}, device_id_type=MESH
        )
        return carry

    lax.fori_loop(1, members, greet, 0)
    pl.semaphore_signal(barrier, inc=1, device_id={"col": 1 - col}, device_id_type=MESH)

    normed[pl.ds(rows * cols, LANES), :] = jnp.zeros((LANES, channels), bf16)

    ones = jnp.ones((channels, channels), bf16)

    def norm_step(b, carry):
        values = rep_ref[pl.ds(b * step_rows, step_rows)].reshape(step_rows * cols, channels)
        average = jnp.dot(values, ones, preferred_element_type=f32) * (1.0 / channels)
        centred = values.astype(f32) - average
        var = jnp.mean(jnp.square(centred), axis=-1, keepdims=True)
        result = centred * lax.rsqrt(var + epsilon) * in_gain_ref[...] + in_bias_ref[...]
        start = pl.multiple_of(b * step_rows * cols, 16)
        normed[pl.ds(start, step_rows * cols), :] = result.astype(bf16)
        return carry

    lax.fori_loop(0, rows // step_rows, norm_step, 0)
    maskf[...] = jnp.zeros_like(maskf)
    maskf[:, 0:cols] = mask_ref[...].astype(f32)
    scaled = format_limit / hist_ref[...]
    flipped = jnp.concatenate([scaled[0:1], scaled[1:2]], axis=1)
    flipped = jnp.broadcast_to(flipped, (channels, channels))
    inverse[...] = jnp.transpose(flipped)
    peak[...] = jnp.zeros_like(peak)
    tail = left_s.shape[0] - half * rows
    left_s[pl.ds(half * rows, tail), :] = jnp.zeros((tail, LANES), f32)
    right_s[pl.ds(half * rows, tail), :] = jnp.zeros((tail, LANES), f32)

    def project(side, target):
        base = side * half

        def one(i):
            block = normed[pl.ds(pl.multiple_of(i * cols, 16), LANES), :]
            p = lax.dot_general(
                proj_ref[2 * base : 2 * base + channels, :],
                block,
                (((1,), (1,)), ((), ())),
                preferred_element_type=f32,
            )
            value = jax.nn.sigmoid(p[half:]) * p[:half] * maskf[pl.ds(i, 1), :]
            target[pl.ds(i, half, stride=rows), :] = jnp.clip(
                value * inverse[base : base + half, :], -format_limit, format_limit
            )
            return jnp.abs(value)

        def step(b, top):
            for u in range(project_rows):
                top = jnp.maximum(top, one(b * project_rows + u))
            return top

        top = lax.fori_loop(0, rows // project_rows, step, jnp.zeros((half, LANES), f32))
        peak[base : base + half, :] = top

    project(1, right_s)
    bounds = [-(-pairs * c // chunks) for c in range(chunks + 1)]

    def z_copy(source, c, direction):
        window = pl.ds(2 * bounds[c], 2 * (bounds[c + 1] - bounds[c]))
        toward = z + 1 - 2 * direction
        return pltpu.make_async_remote_copy(
            src_ref=right_all.at[source, window],
            dst_ref=right_all.at[source, window],
            send_sem=z_send.at[direction, source],
            recv_sem=z_recv.at[source, c],
            device_id={"gx": toward},
            device_id_type=MESH,
        )

    def left_copy(c):
        window = pl.ds(2 * bounds[c], 2 * (bounds[c + 1] - bounds[c]))
        return pltpu.make_async_remote_copy(
            src_ref=left_t.at[window],
            dst_ref=left_r.at[window],
            send_sem=l_send,
            recv_sem=l_recv.at[c],
            device_id={"gx": near},
            device_id_type=MESH,
        )

    pl.semaphore_wait(barrier, members)
    for c in range(chunks):
        for g in range(2 * bounds[c], 2 * bounds[c + 1]):
            tile = jnp.transpose(right_s[g * span : g * span + LANES, :])
            right_all[z, g] = tile[:cols].astype(bf16)

        now = True if c < 2 else jnp.logical_not(is_end)

        @pl.when((z < nz - 1) & now)
        def _():
            z_copy(z, c, 0).start()

        @pl.when((z > 0) & now)
        def _():
            z_copy(z, c, 1).start()

    project(0, left_s)

    @pl.when(is_end)
    def _():
        for c in range(chunks):
            for g in range(2 * bounds[c], 2 * bounds[c + 1]):
                tile = jnp.transpose(left_s[g * span : g * span + LANES, :])
                left_t[g] = tile[:cols].astype(bf16)
            left_copy(c).start()
            if c + 2 < chunks:
                z_copy(z, c + 2, inward).start()

    for g in range(groups):
        left_b[g] = left_s[g * span : g * span + LANES, :].astype(bf16)

    peaks[me] = jnp.broadcast_to(jnp.max(jnp.transpose(peak[...]), axis=0, keepdims=True), (8, channels))

    def spread_peak(t, carry):
        peer = lax.rem(me + t, members)
        pltpu.make_async_remote_copy(
            src_ref=peaks.at[me],
            dst_ref=peaks.at[me],
            send_sem=peak_send,
            recv_sem=peak_recv,
            device_id={"gx": peer // ny, "gy": lax.rem(peer, ny)},
            device_id_type=MESH,
        ).start()
        return carry

    lax.fori_loop(1, members, spread_peak, 0)

    lane = lax.broadcasted_iota(jnp.int32, (rows, LANES), 1)

    def triangle_pair(lhs, r, p):
        halves = []
        for u in range(2):
            res = lax.dot_general(
                lhs[2 * p + u][:, :cols],
                right_all[r, 2 * p + u],
                (((1,), (0,)), ((), ())),
                preferred_element_type=f32,
            )
            t = res[:rows]
            for s in range(1, per):
                t = jnp.where(lane >= s * rows, res[s * rows : (s + 1) * rows], t)
            halves.append(t)
        return jnp.concatenate(halves, axis=0)

    def x_copy(target, sub, c, source):
        window = pl.ds(bounds[c], bounds[c + 1] - bounds[c])
        return pltpu.make_async_remote_copy(
            src_ref=send_t.at[0, target, sub, window],
            dst_ref=recv_t.at[0, source, sub, window],
            send_sem=x_send.at[0, target, sub],
            recv_sem=x_recv.at[0, source, sub, c],
            device_id={"gy": target},
            device_id_type=MESH,
        )

    def far_copy(owner, sub, c, source):
        window = pl.ds(bounds[c], bounds[c + 1] - bounds[c])
        return pltpu.make_async_remote_copy(
            src_ref=send_t.at[1, owner, sub, window],
            dst_ref=recv_t.at[1, source, sub, window],
            send_sem=x_send.at[1, owner, sub],
            recv_sem=x_recv.at[1, source, sub, c],
            device_id={"gx": end, "gy": owner},
            device_id_type=MESH,
        )

    def triangle_block(r, c):
        owner, sub = r // ratio, lax.rem(r, ratio)
        slot = jnp.where(owner == y, sub, ratio)
        for p in range(bounds[c], bounds[c + 1]):
            t = triangle_pair(left_b, r, p)
            own_t[slot, p] = t
            send_t[0, owner, sub, p] = t.astype(bf16)

        @pl.when(owner != y)
        def _():
            x_copy(owner, sub, c, y).start()

    def far_block(r, c):
        owner, sub = r // ratio, lax.rem(r, ratio)
        for p in range(bounds[c], bounds[c + 1]):
            send_t[1, owner, sub, p] = triangle_pair(left_e, r, p).astype(bf16)
        far_copy(owner, sub, c, y).start()

    for c in range(chunks):
        triangle_block(z, c)

    def gate_step(b, carry):
        for u in range(gate_rows):
            i = b * gate_rows + u
            block = normed[pl.ds(pl.multiple_of(i * cols, 16), LANES), :]
            gating[i] = jax.nn.sigmoid(
                lax.dot_general(
                    gate_ref[...], block, (((1,), (1,)), ((), ())), preferred_element_type=f32
                )
            )
        return carry

    lax.fori_loop(0, rows // gate_rows, gate_step, 0)
    group_lane = lax.broadcasted_iota(jnp.int32, (1, LANES), 1)

    def lane_vector(scalar_of, g):
        ch = [jnp.minimum(g * per + s, half - 1) for s in range(per)]
        vector = jnp.full((1, LANES), scalar_of(ch[0]), f32)
        for s in range(1, per):
            vector = jnp.where(group_lane >= s * rows, scalar_of(ch[s]), vector)
        return vector

    def scale_of(ch):
        return (hist_smem[0, ch] / format_limit) * (hist_smem[1, ch] / format_limit)

    def fill_vectors(g, carry):
        vecs[0, pl.ds(g, 1), :] = lane_vector(scale_of, g)
        for cc in range(2):
            vecs[1 + cc, pl.ds(g, 1), :] = lane_vector(lambda ch: out_gain_smem[cc * half + ch], g)
            vecs[3 + cc, pl.ds(g, 1), :] = lane_vector(lambda ch: out_bias_smem[cc * half + ch], g)
        return carry

    lax.fori_loop(0, groups, fill_vectors, 0)

    def pair_vector(v, p):
        parts = [jnp.broadcast_to(vecs[v, 2 * p + u : 2 * p + u + 1, :], (rows, LANES)) for u in range(2)]
        return jnp.concatenate(parts, axis=0)

    def c_copy(sub, c):
        window = pl.ds(bounds[c], bounds[c + 1] - bounds[c])
        return pltpu.make_async_remote_copy(
            src_ref=full_t.at[col, sub, window],
            dst_ref=full_t.at[col, sub, window],
            send_sem=c_send.at[sub],
            recv_sem=c_recv.at[sub, c],
            device_id={"col": 1 - col},
            device_id_type=MESH,
        )

    def finish_block(r, c):
        owner, sub = r // ratio, lax.rem(r, ratio)

        @pl.when(owner == y)
        def _():
            def arrive(t, carry):
                x_copy(y, sub, c, lax.rem(y + t, ny)).wait_recv()
                return carry

            lax.fori_loop(1, ny, arrive, 0)
            for p in range(bounds[c], bounds[c + 1]):
                total = own_t[sub, p]
                for t in range(1, ny):
                    total = total + recv_t[0, lax.rem(y + t, ny), sub, p].astype(f32)
                full_t[col, sub, p] = (total * pair_vector(0, p)).astype(bf16)
            c_copy(sub, c).start()

    row_at = lax.broadcasted_iota(jnp.int32, (2 * rows, LANES), 0) // rows
    lane_at = lax.broadcasted_iota(jnp.int32, (2 * rows, LANES), 1) // rows
    valid = (((pairs - 1) * 2 + row_at) * per + lane_at) < half

    def segment_mean(pair_sum):
        x = pair_sum[:rows] + pair_sum[rows:]
        total = x
        for s in range(1, per):
            total = total + pltpu.roll(x, s * rows, 1)
        result = total
        for s in range(1, per):
            moved = pltpu.roll(total, LANES - s * rows, 1)
            result = jnp.where(lane < (per - s) * rows, moved, result)
        result = result * (1.0 / channels)
        return jnp.concatenate([result, result], axis=0)

    def norm_sub(sub):
        for c in range(chunks):
            c_copy(sub, c).wait_recv()
        total = jnp.zeros((2 * rows, LANES), f32)
        for p in range(pairs):
            total = total + full_t[0, sub, p].astype(f32) + full_t[1, sub, p].astype(f32)
        mean = segment_mean(total)
        squares = jnp.zeros((2 * rows, LANES), f32)
        for p in range(pairs):
            for cc in range(2):
                square = jnp.square(full_t[cc, sub, p].astype(f32) - mean)
                if p == pairs - 1:
                    square = jnp.where(valid, square, 0.0)
                squares = squares + square
        factor = lax.rsqrt(segment_mean(squares) + epsilon)
        for p in range(pairs):
            for cc in range(2):
                t = (full_t[cc, sub, p].astype(f32) - mean) * factor
                t = t * pair_vector(1 + cc, p) + pair_vector(3 + cc, p)
                for ch in range(2 * p * per, min(2 * (p + 1) * per, half)):
                    u, s = ch // per - 2 * p, ch % per
                    piece = t[u * rows : (u + 1) * rows]
                    piece = pltpu.roll(piece, LANES - s * rows, 1) if s else piece
                    at = sub * (rows * pitch) + cc * half + ch
                    spread_t[pl.ds(at, rows, stride=pitch), :] = piece

    first_low = jnp.where(is_end, high_side, 2 * y < ny)
    order = jnp.where(first_low, ratio - 1, 0)
    step_sign = jnp.where(first_low, -1, 1)

    def norm_turn(turn):
        norm_sub(order + step_sign * turn)

    wide = lax.broadcasted_iota(jnp.int32, (half, LANES), 1)

    def mix_turn(turn):
        sub = order + step_sign * turn
        inside = (wide >= sub * rows) & (wide < (sub + 1) * rows)

        def mix_step(b, carry):
            for u in range(mix_rows):
                i = b * mix_rows + u
                tile = spread_t[pl.ds((sub * rows + i) * pitch, channels), :].astype(bf16)
                mixing = jnp.dot(out_weight_ref[...], tile, preferred_element_type=f32)
                mixing = pltpu.roll(mixing, sub * rows, 1)
                if turn:
                    mixing = jnp.where(inside, mixing, mixed[i])
                if turn < ratio - 1:
                    mixed[i] = mixing
                else:
                    out_ref[i] = (gating[i] * mixing)[:, :cols].astype(bf16)
            return carry

        lax.fori_loop(0, rows // mix_rows, mix_step, 0)

    def return_block(r, c):
        owner, sub = r // ratio, lax.rem(r, ratio)

        @pl.when(owner == y)
        def _():
            def arrive(source, carry):
                far_copy(y, sub, c, source).wait_recv()
                return carry

            lax.fori_loop(0, ny, arrive, 0)
            for p in range(bounds[c], bounds[c + 1]):
                total = recv_t[1, 0, sub, p].astype(f32)
                for source in range(1, ny):
                    total = total + recv_t[1, source, sub, p].astype(f32)
                full_t[col, sub, p] = (total * pair_vector(0, p)).astype(bf16)
            c_copy(sub, c).start()

    within = nz == 4 and ratio == 2

    @pl.when(is_next)
    def _():
        end_order = [("right", c) for c in range(min(2, chunks))]
        for c in range(chunks):
            end_order.append(("left", c))
            if c + 2 < chunks:
                end_order.append(("right", c + 2))
        queue = [[(z, c) for c in range(chunks)]]
        held, lefts = [], []
        for s in range(2 * chunks):
            kind, ce = end_order[s]
            k, c = 1 + s // chunks, s % chunks
            source = z - sgn * k
            if kind == "right":
                z_copy(end, ce, inward).wait_recv()
                z_copy(end, ce, inward).start()
            z_copy(source, c, 1 - inward).wait_recv()
            held.append((k, c))
            ready = [(k, c)] if c in lefts else []
            if kind == "left":
                left_copy(ce).wait_recv()
                for g in range(2 * bounds[ce], 2 * bounds[ce + 1]):
                    tile = jnp.concatenate(
                        [left_r[g].astype(f32), jnp.zeros((LANES - cols, LANES), f32)], axis=0
                    )
                    left_e[g] = jnp.transpose(tile).astype(bf16)
                lefts.append(ce)
                ready += [(kk, cc) for kk, cc in held if cc == ce]
            for kk, cc in ready:
                far_block(z - sgn * kk, cc)
            todo = [(source, c)]
            if kind == "right":
                todo.append((end, ce))
            for block in todo:
                triangle_block(*block)
            queue.append(todo)
            if s >= 2:
                for block in queue.pop(0):
                    finish_block(*block)
            if s >= chunks and len(queue) > 2:
                for block in queue.pop(0):
                    finish_block(*block)
        if within:
            norm_turn(0)
        for todo in queue:
            for block in todo:
                finish_block(*block)
        if within:
            mix_turn(0)

        def farther(k, carry):
            for c in range(chunks):
                z_copy(z - sgn * k, c, 1 - inward).wait_recv()
                far_block(z - sgn * k, c)
                triangle_block(z - sgn * k, c)
                finish_block(z - sgn * k, c)
            return carry

        if nz > 4:
            lax.fori_loop(3, nz - 1, farther, 0)

    if nz > 4:

        @pl.when(jnp.logical_not(is_end | is_next))
        def _():
            def ring_step(d, carry):
                for c in range(chunks):
                    for source, direction, there in ((z - d, 0, z - d >= 0), (z + d, 1, z + d < nz)):

                        @pl.when(there)
                        def _(source=source, direction=direction, c=c):
                            z_copy(source, c, direction).wait_recv()
                            z_copy(source, c, direction).start()
                            triangle_block(source, c)
                            finish_block(source, c)

                return carry

            lax.fori_loop(1, nz - 1, ring_step, 0)
            for c in range(chunks):
                finish_block(z, c)

    @pl.when(is_end)
    def _():
        def arrived(source, c):
            z_copy(source, c, 1 - inward).wait_recv()
            triangle_block(source, c)

        def norm_if(here):
            if within:

                @pl.when(here)
                def _():
                    norm_turn(0)

        def farther_back(k, carry):
            for c in range(chunks):
                return_block(near - sgn * k, c)
            return carry

        for c in range(chunks):
            arrived(near, c)
        for c in range(chunks):
            finish_block(z, c)
        norm_if(z // ratio == y)
        for c in range(chunks):
            finish_block(near, c)
        farther_back(1, 0)
        norm_if(z // ratio != y)
        if within:
            mix_turn(0)
        lax.fori_loop(2, nz - 1, farther_back, 0)

    others = peaks.at[pl.ds(0, members - 1)]
    pltpu.make_async_copy(others, others, peak_recv).wait()
    top = jnp.max(jnp.max(peaks[...], axis=0), axis=0, keepdims=True)
    amax_ref[0:1, :] = top[:, :half]
    amax_ref[1:2, :] = top[:, half:]

    pltpu.make_async_copy(others, others, peak_send).wait()

    def sent(ref, sem):
        pltpu.make_async_copy(ref, ref, sem).wait()

    def drain_x(t, carry):
        target = lax.rem(y + t, ny)
        for sub in range(ratio):
            r = target * ratio + sub

            @pl.when(jnp.logical_not(is_end) | (r == z) | (r == near))
            def _(sub=sub):
                sent(send_t.at[0, target, sub], x_send.at[0, target, sub])

        return carry

    lax.fori_loop(1, ny, drain_x, 0)

    def drain_far(r, carry):
        @pl.when((r != end) & (r != z))
        def _():
            owner, sub = r // ratio, lax.rem(r, ratio)
            sent(send_t.at[1, owner, sub], x_send.at[1, owner, sub])

        return carry

    @pl.when(is_next)
    def _():
        lax.fori_loop(0, nz, drain_far, 0)

    @pl.when(is_end)
    def _():
        sent(left_t, l_send)

    def drain_z(source, carry):
        @pl.when((source <= z) & (z < nz - 1) & ((source == z) | (z <= nz - 3)))
        def _():
            sent(right_all.at[source], z_send.at[0, source])

        @pl.when((source >= z) & (z > 0) & ((source == z) | (z >= 2)))
        def _():
            sent(right_all.at[source], z_send.at[1, source])

        return carry

    lax.fori_loop(0, nz, drain_z, 0)

    for turn in range(1 if within else 0, ratio):
        norm_turn(turn)
        mix_turn(turn)

    for sub in range(ratio):
        sent(full_t.at[col, sub], c_send.at[sub])


def on_device(
    nz,
    ny,
    pair_rep,
    pair_mask,
    amax_history,
    in_gain,
    in_bias,
    proj_weight,
    gate_weight,
    out_gain,
    out_bias,
    out_weight,
):
    crops, rows, cols, channels = pair_rep.shape
    half = proj_weight.shape[2]
    chunks = 5
    ratio = nz // ny
    per = LANES // rows
    pairs = -(-half // (2 * per))
    groups = 2 * pairs
    members = nz * ny
    weights = jnp.transpose(proj_weight, (1, 2, 0)).reshape(4 * half, channels)
    scratch_rows = -(-((groups - 1) * per * rows + LANES) // 8) * 8
    dma = pltpu.SemaphoreType.DMA
    vmem = pl.BlockSpec(memory_space=pltpu.VMEM)
    smem = pl.BlockSpec(memory_space=pltpu.SMEM)
    tile = (2 * rows, LANES)
    update, new_amax = pl.pallas_call(
        functools.partial(kernel, (nz, ny, rows, cols, half, chunks)),
        out_shape=(
            pltpu.VMEM((rows, half, cols), bf16),
            pltpu.VMEM((2, half), f32),
        ),
        in_specs=[vmem, vmem, vmem, smem, vmem, vmem, vmem, vmem, smem, smem, vmem],
        out_specs=(vmem, vmem),
        scratch_shapes=[
            pltpu.VMEM((rows * cols + LANES, channels), bf16),
            pltpu.VMEM((rows, LANES), f32),
            pltpu.VMEM((channels, LANES), f32),
            pltpu.VMEM((channels, LANES), f32),
            pltpu.VMEM((scratch_rows, LANES), f32),
            pltpu.VMEM((scratch_rows, LANES), f32),
            pltpu.VMEM((groups, LANES, LANES), bf16),
            pltpu.VMEM((groups, cols, LANES), bf16),
            pltpu.VMEM((groups, cols, LANES), bf16),
            pltpu.VMEM((groups, LANES, LANES), bf16),
            pltpu.VMEM((nz, groups, cols, LANES), bf16),
            pltpu.VMEM((ratio + 1, pairs) + tile, f32),
            pltpu.VMEM((2, ny, ratio, pairs) + tile, bf16),
            pltpu.VMEM((2, ny, ratio, pairs) + tile, bf16),
            pltpu.VMEM((2, ratio, pairs) + tile, bf16),
            pltpu.VMEM((ratio * rows * (channels + 1) + 8, LANES), f32),
            pltpu.VMEM((5, groups, LANES), f32),
            pltpu.VMEM((rows, half, LANES), f32),
            pltpu.VMEM((rows, half, LANES), f32),
            pltpu.VMEM((members, 8, channels), f32),
            dma,
            dma,
            dma((2, nz)),
            dma((nz, chunks)),
            dma,
            dma((chunks,)),
            dma((2, ny, ratio)),
            dma((2, ny, ratio, chunks)),
            dma((ratio,)),
            dma((ratio, chunks)),
        ],
        compiler_params=pltpu.CompilerParams(
            collective_id=0, has_side_effects=True, vmem_limit_bytes=56 * 1024 * 1024
        ),
    )(
        pair_rep[0],
        pair_mask[0],
        amax_history,
        amax_history,
        in_gain.reshape(1, channels),
        in_bias.reshape(1, channels),
        weights,
        gate_weight.T,
        out_gain,
        out_bias,
        out_weight.T,
    )
    return jnp.transpose(update, (0, 2, 1))[None], new_amax


def solution(mesh):
    placed = (
        P("ga", "gx", "gy", None),
        P("ga", "gx", "gy"),
        P(None, "col"),
        P(),
        P(),
        P(None, None, "col"),
        P(None, "col"),
        P(),
        P(),
        P(None, "col"),
    )
    return jax.shard_map(
        functools.partial(on_device, mesh.shape["gx"], mesh.shape["gy"]),
        mesh=mesh,
        in_specs=placed,
        out_specs=(P("ga", "gx", "gy", "col"), P("ga", "col")),
        check_vma=False,
    )
```

```python
import functools

import jax
import jax.numpy as jnp
from jax import lax
from jax.experimental import pallas as pl
from jax.experimental.pallas import tpu as pltpu
from jax.sharding import PartitionSpec as P

epsilon = 1e-05
format_limit = 448.0
LANES = 128
f32, bf16 = jnp.float32, jnp.bfloat16
MESH = pl.DeviceIdType.MESH


def kernel(
    dims,
    rep_ref,
    mask_ref,
    hist_ref,
    hist_smem,
    in_gain_ref,
    in_bias_ref,
    proj_ref,
    gate_ref,
    out_gain_smem,
    out_bias_smem,
    out_weight_ref,
    out_ref,
    amax_ref,
    normed,
    maskf,
    inverse,
    peak,
    left_s,
    right_s,
    left_b,
    left_t,
    left_r,
    left_e,
    right_all,
    own_t,
    send_t,
    recv_t,
    full_t,
    spread_t,
    vecs,
    mixed,
    gating,
    peaks,
    peak_send,
    peak_recv,
    z_send,
    z_recv,
    l_send,
    l_recv,
    x_send,
    x_recv,
    c_send,
    c_recv,
):
    nz, ny, rows, cols, half, chunks = dims
    ratio = nz // ny
    channels = 2 * half
    per = LANES // rows
    pairs = -(-half // (2 * per))
    groups = 2 * pairs
    span = per * rows
    pitch = channels + 1
    z, y, col = lax.axis_index("gx"), lax.axis_index("gy"), lax.axis_index("col")
    members = nz * ny
    me = z * ny + y
    is_end = (z == 0) | (z == nz - 1)
    is_next = (z == 1) | (z == nz - 2)
    high_side = 2 * z >= nz
    sgn = jnp.where(high_side, 1, -1)
    end = jnp.where(high_side, nz - 1, 0)
    inward = jnp.where(high_side, 1, 0)
    near = z - sgn

    def steps(limit):
        return max(u for u in range(1, limit + 1) if rows % u == 0)

    step_rows, project_rows, gate_rows, mix_rows = steps(40), steps(40), steps(40), steps(40)

    barrier = pltpu.get_barrier_semaphore()

    def greet(t, carry):
        peer = lax.rem(me + t, members)
        pl.semaphore_signal(
            barrier, inc=1, device_id={"gx": peer // ny, "gy": lax.rem(peer, ny)}, device_id_type=MESH
        )
        return carry

    lax.fori_loop(1, members, greet, 0)
    pl.semaphore_signal(barrier, inc=1, device_id={"col": 1 - col}, device_id_type=MESH)

    normed[pl.ds(rows * cols, LANES), :] = jnp.zeros((LANES, channels), bf16)

    ones = jnp.ones((channels, channels), bf16)

    def norm_step(b, carry):
        values = rep_ref[pl.ds(b * step_rows, step_rows)].reshape(step_rows * cols, channels)
        average = jnp.dot(values, ones, preferred_element_type=f32) * (1.0 / channels)
        centred = values.astype(f32) - average
        var = jnp.mean(jnp.square(centred), axis=-1, keepdims=True)
        result = centred * lax.rsqrt(var + epsilon) * in_gain_ref[...] + in_bias_ref[...]
        start = pl.multiple_of(b * step_rows * cols, 16)
        normed[pl.ds(start, step_rows * cols), :] = result.astype(bf16)
        return carry

    lax.fori_loop(0, rows // step_rows, norm_step, 0)
    maskf[...] = jnp.zeros_like(maskf)
    maskf[:, 0:cols] = mask_ref[...].astype(f32)
    scaled = format_limit / hist_ref[...]
    flipped = jnp.concatenate([scaled[0:1], scaled[1:2]], axis=1)
    flipped = jnp.broadcast_to(flipped, (channels, channels))
    inverse[...] = jnp.transpose(flipped)
    peak[...] = jnp.zeros_like(peak)
    tail = left_s.shape[0] - half * rows
    left_s[pl.ds(half * rows, tail), :] = jnp.zeros((tail, LANES), f32)
    right_s[pl.ds(half * rows, tail), :] = jnp.zeros((tail, LANES), f32)

    def project(side, target):
        base = side * half

        def one(i):
            block = normed[pl.ds(pl.multiple_of(i * cols, 16), LANES), :]
            p = lax.dot_general(
                proj_ref[2 * base : 2 * base + channels, :],
                block,
                (((1,), (1,)), ((), ())),
                preferred_element_type=f32,
            )
            value = jax.nn.sigmoid(p[half:]) * p[:half] * maskf[pl.ds(i, 1), :]
            target[pl.ds(i, half, stride=rows), :] = jnp.clip(
                value * inverse[base : base + half, :], -format_limit, format_limit
            )
            return jnp.abs(value)

        def step(b, top):
            for u in range(project_rows):
                top = jnp.maximum(top, one(b * project_rows + u))
            return top

        top = lax.fori_loop(0, rows // project_rows, step, jnp.zeros((half, LANES), f32))
        peak[base : base + half, :] = top

    project(1, right_s)
    bounds = [-(-pairs * c // chunks) for c in range(chunks + 1)]

    def z_copy(source, c, direction):
        window = pl.ds(2 * bounds[c], 2 * (bounds[c + 1] - bounds[c]))
        toward = z + 1 - 2 * direction
        return pltpu.make_async_remote_copy(
            src_ref=right_all.at[source, window],
            dst_ref=right_all.at[source, window],
            send_sem=z_send.at[direction, source],
            recv_sem=z_recv.at[source, c],
            device_id={"gx": toward},
            device_id_type=MESH,
        )

    def left_copy(c):
        window = pl.ds(2 * bounds[c], 2 * (bounds[c + 1] - bounds[c]))
        return pltpu.make_async_remote_copy(
            src_ref=left_t.at[window],
            dst_ref=left_r.at[window],
            send_sem=l_send,
            recv_sem=l_recv.at[c],
            device_id={"gx": near},
            device_id_type=MESH,
        )

    pl.semaphore_wait(barrier, members)
    for c in range(chunks):
        for g in range(2 * bounds[c], 2 * bounds[c + 1]):
            tile = jnp.transpose(right_s[g * span : g * span + LANES, :])
            right_all[z, g] = tile[:cols].astype(bf16)

        now = True if c < 2 else jnp.logical_not(is_end)

        @pl.when((z < nz - 1) & now)
        def _():
            z_copy(z, c, 0).start()

        @pl.when((z > 0) & now)
        def _():
            z_copy(z, c, 1).start()

    project(0, left_s)

    @pl.when(is_end)
    def _():
        for c in range(chunks):
            for g in range(2 * bounds[c], 2 * bounds[c + 1]):
                tile = jnp.transpose(left_s[g * span : g * span + LANES, :])
                left_t[g] = tile[:cols].astype(bf16)
            left_copy(c).start()
            if c + 2 < chunks:
                z_copy(z, c + 2, inward).start()

    for g in range(groups):
        left_b[g] = left_s[g * span : g * span + LANES, :].astype(bf16)

    peaks[me] = jnp.broadcast_to(jnp.max(jnp.transpose(peak[...]), axis=0, keepdims=True), (8, channels))

    def spread_peak(t, carry):
        peer = lax.rem(me + t, members)
        pltpu.make_async_remote_copy(
            src_ref=peaks.at[me],
            dst_ref=peaks.at[me],
            send_sem=peak_send,
            recv_sem=peak_recv,
            device_id={"gx": peer // ny, "gy": lax.rem(peer, ny)},
            device_id_type=MESH,
        ).start()
        return carry

    lax.fori_loop(1, members, spread_peak, 0)

    lane = lax.broadcasted_iota(jnp.int32, (rows, LANES), 1)

    def triangle_pair(lhs, r, p):
        halves = []
        for u in range(2):
            res = lax.dot_general(
                lhs[2 * p + u][:, :cols],
                right_all[r, 2 * p + u],
                (((1,), (0,)), ((), ())),
                preferred_element_type=f32,
            )
            t = res[:rows]
            for s in range(1, per):
                t = jnp.where(lane >= s * rows, res[s * rows : (s + 1) * rows], t)
            halves.append(t)
        return jnp.concatenate(halves, axis=0)

    def x_copy(target, sub, c, source):
        window = pl.ds(bounds[c], bounds[c + 1] - bounds[c])
        return pltpu.make_async_remote_copy(
            src_ref=send_t.at[0, target, sub, window],
            dst_ref=recv_t.at[0, source, sub, window],
            send_sem=x_send.at[0, target, sub],
            recv_sem=x_recv.at[0, source, sub, c],
            device_id={"gy": target},
            device_id_type=MESH,
        )

    def far_copy(owner, sub, c, source):
        window = pl.ds(bounds[c], bounds[c + 1] - bounds[c])
        return pltpu.make_async_remote_copy(
            src_ref=send_t.at[1, owner, sub, window],
            dst_ref=recv_t.at[1, source, sub, window],
            send_sem=x_send.at[1, owner, sub],
            recv_sem=x_recv.at[1, source, sub, c],
            device_id={"gx": end, "gy": owner},
            device_id_type=MESH,
        )

    def triangle_block(r, c):
        owner, sub = r // ratio, lax.rem(r, ratio)
        slot = jnp.where(owner == y, sub, ratio)
        for p in range(bounds[c], bounds[c + 1]):
            t = triangle_pair(left_b, r, p)
            own_t[slot, p] = t
            send_t[0, owner, sub, p] = t.astype(bf16)

        @pl.when(owner != y)
        def _():
            x_copy(owner, sub, c, y).start()

    def far_block(r, c):
        owner, sub = r // ratio, lax.rem(r, ratio)
        for p in range(bounds[c], bounds[c + 1]):
            send_t[1, owner, sub, p] = triangle_pair(left_e, r, p).astype(bf16)
        far_copy(owner, sub, c, y).start()

    for c in range(chunks):
        triangle_block(z, c)

    def gate_step(b, carry):
        for u in range(gate_rows):
            i = b * gate_rows + u
            block = normed[pl.ds(pl.multiple_of(i * cols, 16), LANES), :]
            gating[i] = jax.nn.sigmoid(
                lax.dot_general(
                    gate_ref[...], block, (((1,), (1,)), ((), ())), preferred_element_type=f32
                )
            )
        return carry

    lax.fori_loop(0, rows // gate_rows, gate_step, 0)
    group_lane = lax.broadcasted_iota(jnp.int32, (1, LANES), 1)

    def lane_vector(scalar_of, g):
        ch = [jnp.minimum(g * per + s, half - 1) for s in range(per)]
        vector = jnp.full((1, LANES), scalar_of(ch[0]), f32)
        for s in range(1, per):
            vector = jnp.where(group_lane >= s * rows, scalar_of(ch[s]), vector)
        return vector

    def scale_of(ch):
        return (hist_smem[0, ch] / format_limit) * (hist_smem[1, ch] / format_limit)

    def fill_vectors(g, carry):
        vecs[0, pl.ds(g, 1), :] = lane_vector(scale_of, g)
        for cc in range(2):
            vecs[1 + cc, pl.ds(g, 1), :] = lane_vector(lambda ch: out_gain_smem[cc * half + ch], g)
            vecs[3 + cc, pl.ds(g, 1), :] = lane_vector(lambda ch: out_bias_smem[cc * half + ch], g)
        return carry

    lax.fori_loop(0, groups, fill_vectors, 0)

    def pair_vector(v, p):
        parts = [jnp.broadcast_to(vecs[v, 2 * p + u : 2 * p + u + 1, :], (rows, LANES)) for u in range(2)]
        return jnp.concatenate(parts, axis=0)

    def c_copy(sub, c):
        window = pl.ds(bounds[c], bounds[c + 1] - bounds[c])
        return pltpu.make_async_remote_copy(
            src_ref=full_t.at[col, sub, window],
            dst_ref=full_t.at[col, sub, window],
            send_sem=c_send.at[sub],
            recv_sem=c_recv.at[sub, c],
            device_id={"col": 1 - col},
            device_id_type=MESH,
        )

    def finish_block(r, c):
        owner, sub = r // ratio, lax.rem(r, ratio)

        @pl.when(owner == y)
        def _():
            def arrive(t, carry):
                x_copy(y, sub, c, lax.rem(y + t, ny)).wait_recv()
                return carry

            lax.fori_loop(1, ny, arrive, 0)
            for p in range(bounds[c], bounds[c + 1]):
                total = own_t[sub, p]
                for t in range(1, ny):
                    total = total + recv_t[0, lax.rem(y + t, ny), sub, p].astype(f32)
                full_t[col, sub, p] = (total * pair_vector(0, p)).astype(bf16)
            c_copy(sub, c).start()

    row_at = lax.broadcasted_iota(jnp.int32, (2 * rows, LANES), 0) // rows
    lane_at = lax.broadcasted_iota(jnp.int32, (2 * rows, LANES), 1) // rows
    valid = (((pairs - 1) * 2 + row_at) * per + lane_at) < half

    def segment_mean(pair_sum):
        x = pair_sum[:rows] + pair_sum[rows:]
        total = x
        for s in range(1, per):
            total = total + pltpu.roll(x, s * rows, 1)
        result = total
        for s in range(1, per):
            moved = pltpu.roll(total, LANES - s * rows, 1)
            result = jnp.where(lane < (per - s) * rows, moved, result)
        result = result * (1.0 / channels)
        return jnp.concatenate([result, result], axis=0)

    def norm_sub(sub):
        for c in range(chunks):
            c_copy(sub, c).wait_recv()
        total = jnp.zeros((2 * rows, LANES), f32)
        for p in range(pairs):
            total = total + full_t[0, sub, p].astype(f32) + full_t[1, sub, p].astype(f32)
        mean = segment_mean(total)
        squares = jnp.zeros((2 * rows, LANES), f32)
        for p in range(pairs):
            for cc in range(2):
                square = jnp.square(full_t[cc, sub, p].astype(f32) - mean)
                if p == pairs - 1:
                    square = jnp.where(valid, square, 0.0)
                squares = squares + square
        factor = lax.rsqrt(segment_mean(squares) + epsilon)
        for p in range(pairs):
            for cc in range(2):
                t = (full_t[cc, sub, p].astype(f32) - mean) * factor
                t = t * pair_vector(1 + cc, p) + pair_vector(3 + cc, p)
                for ch in range(2 * p * per, min(2 * (p + 1) * per, half)):
                    u, s = ch // per - 2 * p, ch % per
                    piece = t[u * rows : (u + 1) * rows]
                    piece = pltpu.roll(piece, LANES - s * rows, 1) if s else piece
                    at = sub * (rows * pitch) + cc * half + ch
                    spread_t[pl.ds(at, rows, stride=pitch), :] = piece

    first_low = jnp.where(is_end, high_side, 2 * y < ny)
    order = jnp.where(first_low, ratio - 1, 0)
    step_sign = jnp.where(first_low, -1, 1)

    def norm_turn(turn):
        norm_sub(order + step_sign * turn)

    wide = lax.broadcasted_iota(jnp.int32, (half, LANES), 1)

    def mix_turn(turn):
        sub = order + step_sign * turn
        inside = (wide >= sub * rows) & (wide < (sub + 1) * rows)

        def mix_step(b, carry):
            for u in range(mix_rows):
                i = b * mix_rows + u
                tile = spread_t[pl.ds((sub * rows + i) * pitch, channels), :].astype(bf16)
                mixing = jnp.dot(out_weight_ref[...], tile, preferred_element_type=f32)
                mixing = pltpu.roll(mixing, sub * rows, 1)
                if turn:
                    mixing = jnp.where(inside, mixing, mixed[i])
                if turn < ratio - 1:
                    mixed[i] = mixing
                else:
                    out_ref[i] = (gating[i] * mixing)[:, :cols].astype(bf16)
            return carry

        lax.fori_loop(0, rows // mix_rows, mix_step, 0)

    def return_block(r, c):
        owner, sub = r // ratio, lax.rem(r, ratio)

        @pl.when(owner == y)
        def _():
            def arrive(source, carry):
                far_copy(y, sub, c, source).wait_recv()
                return carry

            lax.fori_loop(0, ny, arrive, 0)
            for p in range(bounds[c], bounds[c + 1]):
                total = recv_t[1, 0, sub, p].astype(f32)
                for source in range(1, ny):
                    total = total + recv_t[1, source, sub, p].astype(f32)
                full_t[col, sub, p] = (total * pair_vector(0, p)).astype(bf16)
            c_copy(sub, c).start()

    within = nz == 4 and ratio == 2

    @pl.when(is_next)
    def _():
        end_order = [("right", c) for c in range(min(2, chunks))]
        for c in range(chunks):
            end_order.append(("left", c))
            if c + 2 < chunks:
                end_order.append(("right", c + 2))
        queue = [[(z, c) for c in range(chunks)]]
        held, lefts = [], []
        for s in range(2 * chunks):
            kind, ce = end_order[s]
            k, c = 1 + s // chunks, s % chunks
            source = z - sgn * k
            if kind == "right":
                z_copy(end, ce, inward).wait_recv()
                z_copy(end, ce, inward).start()
            z_copy(source, c, 1 - inward).wait_recv()
            held.append((k, c))
            ready = [(k, c)] if c in lefts else []
            if kind == "left":
                left_copy(ce).wait_recv()
                for g in range(2 * bounds[ce], 2 * bounds[ce + 1]):
                    tile = jnp.concatenate(
                        [left_r[g].astype(f32), jnp.zeros((LANES - cols, LANES), f32)], axis=0
                    )
                    left_e[g] = jnp.transpose(tile).astype(bf16)
                lefts.append(ce)
                ready += [(kk, cc) for kk, cc in held if cc == ce]
            for kk, cc in ready:
                far_block(z - sgn * kk, cc)
            todo = [(source, c)]
            if kind == "right":
                todo.append((end, ce))
            for block in todo:
                triangle_block(*block)
            queue.append(todo)
            if s >= 2:
                for block in queue.pop(0):
                    finish_block(*block)
            if s >= chunks and len(queue) > 2:
                for block in queue.pop(0):
                    finish_block(*block)
        if within:
            norm_turn(0)
        for todo in queue:
            for block in todo:
                finish_block(*block)
        if within:
            mix_turn(0)

        def farther(k, carry):
            for c in range(chunks):
                z_copy(z - sgn * k, c, 1 - inward).wait_recv()
                far_block(z - sgn * k, c)
                triangle_block(z - sgn * k, c)
                finish_block(z - sgn * k, c)
            return carry

        if nz > 4:
            lax.fori_loop(3, nz - 1, farther, 0)

    if nz > 4:

        @pl.when(jnp.logical_not(is_end | is_next))
        def _():
            def ring_step(d, carry):
                for c in range(chunks):
                    for source, direction, there in ((z - d, 0, z - d >= 0), (z + d, 1, z + d < nz)):

                        @pl.when(there)
                        def _(source=source, direction=direction, c=c):
                            z_copy(source, c, direction).wait_recv()
                            z_copy(source, c, direction).start()
                            triangle_block(source, c)
                            finish_block(source, c)

                return carry

            lax.fori_loop(1, nz - 1, ring_step, 0)
            for c in range(chunks):
                finish_block(z, c)

    @pl.when(is_end)
    def _():
        def arrived(source, c):
            z_copy(source, c, 1 - inward).wait_recv()
            triangle_block(source, c)

        def norm_if(here):
            if within:

                @pl.when(here)
                def _():
                    norm_turn(0)

        def farther_back(k, carry):
            for c in range(chunks):
                return_block(near - sgn * k, c)
            return carry

        for c in range(chunks):
            arrived(near, c)
        for c in range(chunks):
            finish_block(z, c)
        norm_if(z // ratio == y)
        for c in range(chunks):
            finish_block(near, c)
        lax.fori_loop(1, nz - 1, farther_back, 0)
        norm_if(z // ratio != y)
        if within:
            mix_turn(0)

    others = peaks.at[pl.ds(0, members - 1)]
    pltpu.make_async_copy(others, others, peak_recv).wait()
    top = jnp.max(jnp.max(peaks[...], axis=0), axis=0, keepdims=True)
    amax_ref[0:1, :] = top[:, :half]
    amax_ref[1:2, :] = top[:, half:]

    pltpu.make_async_copy(others, others, peak_send).wait()

    def sent(ref, sem):
        pltpu.make_async_copy(ref, ref, sem).wait()

    def drain_x(t, carry):
        target = lax.rem(y + t, ny)
        for sub in range(ratio):
            r = target * ratio + sub

            @pl.when(jnp.logical_not(is_end) | (r == z) | (r == near))
            def _(sub=sub):
                sent(send_t.at[0, target, sub], x_send.at[0, target, sub])

        return carry

    lax.fori_loop(1, ny, drain_x, 0)

    def drain_far(r, carry):
        @pl.when((r != end) & (r != z))
        def _():
            owner, sub = r // ratio, lax.rem(r, ratio)
            sent(send_t.at[1, owner, sub], x_send.at[1, owner, sub])

        return carry

    @pl.when(is_next)
    def _():
        lax.fori_loop(0, nz, drain_far, 0)

    @pl.when(is_end)
    def _():
        sent(left_t, l_send)

    def drain_z(source, carry):
        @pl.when((source <= z) & (z < nz - 1) & ((source == z) | (z <= nz - 3)))
        def _():
            sent(right_all.at[source], z_send.at[0, source])

        @pl.when((source >= z) & (z > 0) & ((source == z) | (z >= 2)))
        def _():
            sent(right_all.at[source], z_send.at[1, source])

        return carry

    lax.fori_loop(0, nz, drain_z, 0)

    for turn in range(1 if within else 0, ratio):
        norm_turn(turn)
        mix_turn(turn)

    for sub in range(ratio):
        sent(full_t.at[col, sub], c_send.at[sub])


def on_device(
    nz,
    ny,
    pair_rep,
    pair_mask,
    amax_history,
    in_gain,
    in_bias,
    proj_weight,
    gate_weight,
    out_gain,
    out_bias,
    out_weight,
):
    crops, rows, cols, channels = pair_rep.shape
    half = proj_weight.shape[2]
    chunks = 5
    ratio = nz // ny
    per = LANES // rows
    pairs = -(-half // (2 * per))
    groups = 2 * pairs
    members = nz * ny
    weights = jnp.transpose(proj_weight, (1, 2, 0)).reshape(4 * half, channels)
    scratch_rows = -(-((groups - 1) * per * rows + LANES) // 8) * 8
    dma = pltpu.SemaphoreType.DMA
    vmem = pl.BlockSpec(memory_space=pltpu.VMEM)
    smem = pl.BlockSpec(memory_space=pltpu.SMEM)
    tile = (2 * rows, LANES)
    update, new_amax = pl.pallas_call(
        functools.partial(kernel, (nz, ny, rows, cols, half, chunks)),
        out_shape=(
            pltpu.VMEM((rows, half, cols), bf16),
            pltpu.VMEM((2, half), f32),
        ),
        in_specs=[vmem, vmem, vmem, smem, vmem, vmem, vmem, vmem, smem, smem, vmem],
        out_specs=(vmem, vmem),
        scratch_shapes=[
            pltpu.VMEM((rows * cols + LANES, channels), bf16),
            pltpu.VMEM((rows, LANES), f32),
            pltpu.VMEM((channels, LANES), f32),
            pltpu.VMEM((channels, LANES), f32),
            pltpu.VMEM((scratch_rows, LANES), f32),
            pltpu.VMEM((scratch_rows, LANES), f32),
            pltpu.VMEM((groups, LANES, LANES), bf16),
            pltpu.VMEM((groups, cols, LANES), bf16),
            pltpu.VMEM((groups, cols, LANES), bf16),
            pltpu.VMEM((groups, LANES, LANES), bf16),
            pltpu.VMEM((nz, groups, cols, LANES), bf16),
            pltpu.VMEM((ratio + 1, pairs) + tile, f32),
            pltpu.VMEM((2, ny, ratio, pairs) + tile, bf16),
            pltpu.VMEM((2, ny, ratio, pairs) + tile, bf16),
            pltpu.VMEM((2, ratio, pairs) + tile, bf16),
            pltpu.VMEM((ratio * rows * (channels + 1) + 8, LANES), f32),
            pltpu.VMEM((5, groups, LANES), f32),
            pltpu.VMEM((rows, half, LANES), f32),
            pltpu.VMEM((rows, half, LANES), f32),
            pltpu.VMEM((members, 8, channels), f32),
            dma,
            dma,
            dma((2, nz)),
            dma((nz, chunks)),
            dma,
            dma((chunks,)),
            dma((2, ny, ratio)),
            dma((2, ny, ratio, chunks)),
            dma((ratio,)),
            dma((ratio, chunks)),
        ],
        compiler_params=pltpu.CompilerParams(
            collective_id=0, has_side_effects=True, vmem_limit_bytes=56 * 1024 * 1024
        ),
    )(
        pair_rep[0],
        pair_mask[0],
        amax_history,
        amax_history,
        in_gain.reshape(1, channels),
        in_bias.reshape(1, channels),
        weights,
        gate_weight.T,
        out_gain,
        out_bias,
        out_weight.T,
    )
    return jnp.transpose(update, (0, 2, 1))[None], new_amax


def solution(mesh):
    placed = (
        P("ga", "gx", "gy", None),
        P("ga", "gx", "gy"),
        P(None, "col"),
        P(),
        P(),
        P(None, None, "col"),
        P(None, "col"),
        P(),
        P(),
        P(None, "col"),
    )
    return jax.shard_map(
        functools.partial(on_device, mesh.shape["gx"], mesh.shape["gy"]),
        mesh=mesh,
        in_specs=placed,
        out_specs=(P("ga", "gx", "gy", "col"), P("ga", "col")),
        check_vma=False,
    )
```
